8 devices in a mesh: dp: 2 (over z, y), cp: 4 (over x, core).
Axes of the slice: x: 2, y: 2, z: 1, core: 2. Of those that a mesh axis runs over, the one named last changes fastest.
Arguments:
- x: bfloat16 [1024, 2048], P(('dp', 'cp')), parts along dimension 0
- k_cache: bfloat16 [32768, 8, 128], P(('dp', 'cp')), parts along dimension 0
- v_cache: bfloat16 [32768, 8, 128], P(('dp', 'cp')), parts along dimension 0
- ln_gain: bfloat16 [2048], replicated
- w_q: bfloat16 [2048, 2048], replicated
- w_k: bfloat16 [2048, 1024], replicated
- w_v: bfloat16 [2048, 1024], replicated
- w_o: bfloat16 [2048, 2048], replicated
- q_gain: bfloat16 [128], replicated
- k_gain: bfloat16 [128], replicated
Outputs:
- output 1: bfloat16 [1024, 2048], P(('dp', 'cp')), parts along dimension 0
- output 2: bfloat16 [1024, 8, 128], P(('dp', 'cp')), parts along dimension 0
- output 3: bfloat16 [1024, 8, 128], P(('dp', 'cp')), parts along dimension 0
There are 2 independent parts. The reference program is written for one: setup_inputs(seed, part) draws one part's arguments, and reference() takes and returns one part's arrays. A program takes and returns all parts, laid end to end along the dimension named above; an argument that names none is the same for every part.
All inputs are finite; a program needn't handle non-finite values.
Results may differ from the reference program's by a relative error of at most 0.0121848.
Values are sent between devices in bfloat16 or wider.
A program may use at most 1 GiB of HBM per device.

```python
import jax
import jax.numpy as jnp
from jax import lax

HIDDEN = 2048
Q_HEADS = 16
KV_HEADS = 8
HEAD_DIM = 128
NEW_LEN = 512
PREFIX_LEN = 16384
ROW_BLOCK = 16
ROPE_THETA = 1.0e6
NORM_EPS = 1.0e-6


def setup_inputs(seed: int = 0, part: int = 0) -> dict:
    part_key = jax.random.fold_in(jax.random.key(seed), part)
    part_keys = jax.random.split(part_key, 3)
    shared = jax.random.split(jax.random.key(seed + 1), 7)
    q_width = Q_HEADS * HEAD_DIM
    kv_width = KV_HEADS * HEAD_DIM
    total_len = PREFIX_LEN + NEW_LEN
    x = jax.random.normal(part_keys[0], (NEW_LEN, HIDDEN), jnp.float32)
    k_cache = jax.random.normal(part_keys[1], (PREFIX_LEN, KV_HEADS, HEAD_DIM), jnp.float32)
    v_cache = jax.random.normal(part_keys[2], (PREFIX_LEN, KV_HEADS, HEAD_DIM), jnp.float32)
    ln_gain = 1.0 + 0.4 * jax.random.normal(shared[0], (HIDDEN,), jnp.float32)
    w_q = jax.random.normal(shared[1], (HIDDEN, q_width), jnp.float32) * HIDDEN ** -0.5
    w_k = jax.random.normal(shared[2], (HIDDEN, kv_width), jnp.float32) * HIDDEN ** -0.5
    w_v = jax.random.normal(shared[3], (HIDDEN, kv_width), jnp.float32) * HIDDEN ** -0.5
    w_o = jax.random.normal(shared[4], (q_width, HIDDEN), jnp.float32) * (0.5 * (total_len / q_width) ** 0.5)
    q_gain = 1.0 + 0.3 * jax.random.normal(shared[5], (HEAD_DIM,), jnp.float32)
    k_gain = 1.5 + 0.3 * jax.random.normal(shared[6], (HEAD_DIM,), jnp.float32)
    return {'x': x.astype(jnp.bfloat16), 'k_cache': k_cache.astype(jnp.bfloat16), 'v_cache': v_cache.astype(jnp.bfloat16), 'ln_gain': ln_gain.astype(jnp.bfloat16), 'w_q': w_q.astype(jnp.bfloat16), 'w_k': w_k.astype(jnp.bfloat16), 'w_v': w_v.astype(jnp.bfloat16), 'w_o': w_o.astype(jnp.bfloat16), 'q_gain': q_gain.astype(jnp.bfloat16), 'k_gain': k_gain.astype(jnp.bfloat16)}


def rms_norm(vals, gain):
    mean_sq = jnp.mean(vals * vals, axis=-1, keepdims=True)
    return vals * lax.rsqrt(mean_sq + NORM_EPS) * gain


def apply_rope(vals, positions):
    half = HEAD_DIM // 2
    inv_freq = ROPE_THETA ** (-jnp.arange(half, dtype=jnp.float32) * (2.0 / HEAD_DIM))
    angles = positions.astype(jnp.float32)[:, None] * inv_freq[None, :]
    cos_tab = jnp.cos(angles)[:, None, :]
    sin_tab = jnp.sin(angles)[:, None, :]
    first = vals[..., :half]
    second = vals[..., half:]
    return jnp.concatenate([first * cos_tab - second * sin_tab, second * cos_tab + first * sin_tab], axis=-1)


def reference(x, k_cache, v_cache, ln_gain, w_q, w_k, w_v, w_o, q_gain, k_gain):
    group = Q_HEADS // KV_HEADS
    scale = HEAD_DIM ** -0.5
    x_wide = x.astype(jnp.float32)
    hidden = rms_norm(x_wide, ln_gain.astype(jnp.float32)).astype(jnp.bfloat16)
    q_raw = jnp.dot(hidden, w_q, preferred_element_type=jnp.float32).astype(jnp.bfloat16)
    k_raw = jnp.dot(hidden, w_k, preferred_element_type=jnp.float32).astype(jnp.bfloat16)
    v_new = jnp.dot(hidden, w_v, preferred_element_type=jnp.float32).astype(jnp.bfloat16).reshape(NEW_LEN, KV_HEADS, HEAD_DIM)
    positions = PREFIX_LEN + jnp.arange(NEW_LEN)
    q_rot = apply_rope(rms_norm(q_raw.reshape(NEW_LEN, Q_HEADS, HEAD_DIM).astype(jnp.float32), q_gain.astype(jnp.float32)), positions).astype(jnp.bfloat16)
    k_new = apply_rope(rms_norm(k_raw.reshape(NEW_LEN, KV_HEADS, HEAD_DIM).astype(jnp.float32), k_gain.astype(jnp.float32)), positions).astype(jnp.bfloat16)
    keys_all = jnp.concatenate([k_cache, k_new], axis=0).astype(jnp.float32)
    values_all = jnp.concatenate([v_cache, v_new], axis=0).astype(jnp.float32)
    key_pos = jnp.arange(PREFIX_LEN + NEW_LEN)
    block_count = NEW_LEN // ROW_BLOCK
    q_blocks = q_rot.reshape(block_count, ROW_BLOCK, KV_HEADS, group, HEAD_DIM)

    def block_attend(block):
        q_block, block_index = block
        row_pos = PREFIX_LEN + block_index * ROW_BLOCK + jnp.arange(ROW_BLOCK)
        scores = jnp.einsum('rkgd,skd->rkgs', q_block.astype(jnp.float32), keys_all) * scale
        allowed = key_pos[None, :] <= row_pos[:, None]
        scores = jnp.where(allowed[:, None, None, :], scores, -jnp.inf)
        peak = jnp.max(scores, axis=-1, keepdims=True)
        weights = jnp.exp(scores - peak)
        probs = weights / jnp.sum(weights, axis=-1, keepdims=True)
        return jnp.einsum('rkgs,skd->rkgd', probs, values_all)

    attended = lax.map(block_attend, (q_blocks, jnp.arange(block_count)))
    attended = attended.reshape(NEW_LEN, Q_HEADS * HEAD_DIM).astype(jnp.bfloat16)
    out = (x_wide + jnp.dot(attended, w_o, preferred_element_type=jnp.float32)).astype(jnp.bfloat16)
    return (out, k_new, v_new)
```

```python
import functools
import math

import jax
import jax.numpy as jnp
from jax import lax
from jax.experimental import pallas as pl
from jax.experimental.pallas import tpu as pltpu
from jax.sharding import PartitionSpec as P

HEAD_DIM = 128
ROPE_THETA = 1.0e6
NORM_EPS = 1.0e-6
SCALE_LOG2 = HEAD_DIM ** -0.5 * math.log2(math.e)
F32, BF16 = jnp.float32, jnp.bfloat16
MESH = pl.DeviceIdType.MESH

KEY_TILE = 256
PREP = 256
GROUP = 8
LEAD = 3


def rms_norm(vals, gain):
    mean_sq = jnp.mean(vals * vals, axis=-1, keepdims=True)
    return vals * lax.rsqrt(mean_sq + NORM_EPS) * gain


def apply_rope(vals, positions):
    half = HEAD_DIM // 2
    inv_freq = ROPE_THETA ** (-jnp.arange(half, dtype=F32) * (2.0 / HEAD_DIM))
    angles = positions.astype(F32)[:, None] * inv_freq[None, :]
    cos_tab = jnp.cos(angles)[:, None, :]
    sin_tab = jnp.sin(angles)[:, None, :]
    first = vals[..., :half]
    second = vals[..., half:]
    return jnp.concatenate([first * cos_tab - second * sin_tab, second * cos_tab + first * sin_tab], axis=-1)


def project_rows(x_wide, ln_gain, w_q, w_k, w_v, q_gain, k_gain, positions):
    rows = x_wide.shape[0]
    hidden = rms_norm(x_wide, ln_gain.astype(F32)).astype(BF16)
    q_raw = jnp.dot(hidden, w_q, preferred_element_type=F32).astype(BF16).reshape(rows, -1, HEAD_DIM)
    k_raw = jnp.dot(hidden, w_k, preferred_element_type=F32).astype(BF16).reshape(rows, -1, HEAD_DIM)
    v_new = jnp.dot(hidden, w_v, preferred_element_type=F32).astype(BF16).reshape(rows, -1, HEAD_DIM)
    q_rot = apply_rope(rms_norm(q_raw.astype(F32), q_gain.astype(F32)), positions).astype(BF16)
    k_new = apply_rope(rms_norm(k_raw.astype(F32), k_gain.astype(F32)), positions).astype(BF16)
    return q_rot, k_new, v_new


def attend_kernel(n_keys, heads, q_own, k_new, v_new, k_hbm, v_hbm, att_ref,
                  kh, vt, sA, sB, sN, mbuf, lbuf, mcb, obuf, q_recv, part, sib_recv, comb, mir_recv, raw, wide,
                  copy_sem, q_send, q_sem, sib_send, sib_sem, mir_send, mir_sem):
    SB = (sA, sB)
    me = lax.axis_index("cp")
    sibling = me + 1 - 2 * lax.rem(me, 2)
    mirror = lax.rem(me + 2, 4)
    rows = 128
    tiles = n_keys // KEY_TILE
    units = 2 * heads
    TS = lambda t: slice(t * 256, (t + 1) * 256)

    def remote(src, dst, send, recv, to):
        return pltpu.make_async_remote_copy(src_ref=src, dst_ref=dst, send_sem=send, recv_sem=recv,
                                            device_id={"cp": to}, device_id_type=MESH)

    def cache_copy(i, which, slot):
        src = (k_hbm, v_hbm)[which]
        n = PREP * heads
        return pltpu.make_async_copy(src.at[pl.ds(pl.multiple_of(i * n, n), n), :], raw.at[which, slot], copy_sem.at[which, slot])

    for s in range(2):
        cache_copy(s, 0, s).start()
        cache_copy(s, 1, s).start()

    barrier = pltpu.get_barrier_semaphore()
    for peer in (sibling, mirror):
        pl.semaphore_signal(barrier, inc=1, device_id={"cp": peer}, device_id_type=MESH)
    pl.semaphore_wait(barrier, 2)

    def q_to_sibling(g):
        return remote(q_own.at[g], q_recv.at[0, g], q_send.at[0, g], q_sem.at[0, g], sibling)
    def q_to_mirror(g):
        return remote(q_own.at[g], q_recv.at[1, g], q_send.at[1, g], q_sem.at[1, g], mirror)
    def q_forward(g):
        return remote(q_recv.at[1, g], q_recv.at[2, g], q_send.at[2, g], q_sem.at[2, g], sibling)
    for g in range(heads):
        q_to_mirror(g).start()
    for g in range(heads):
        q_to_sibling(g).start()

    def prep(i, _):
        slot = lax.rem(i, 2)
        row = pl.ds(pl.multiple_of(i * PREP, PREP), PREP)
        cache_copy(i, 0, slot).wait()
        wide[0] = raw[0, slot].astype(F32)
        for h in range(heads):
            kh[h, row, :] = wide[0, pl.ds(h, PREP, stride=heads), :].astype(BF16)
        cache_copy(i, 1, slot).wait()
        wide[1] = raw[1, slot].astype(F32)
        for h in range(heads):
            vt[h, :, row] = wide[1, pl.ds(h, PREP, stride=heads), :].T.astype(BF16)
        @pl.when(i + 2 < n_keys // PREP)
        def _():
            cache_copy(i + 2, 0, slot).start()
            cache_copy(i + 2, 1, slot).start()
        return 0
    lax.fori_loop(0, n_keys // PREP, prep, 0)

    for g in range(heads):
        q_to_mirror(g).wait_recv()
        q_forward(g).start()
    for g in range(heads):
        q_to_sibling(g).wait_recv()
        q_forward(g).wait_recv()

    def sib_copy(kind, g):
        return remote(part.at[kind, g, 1], sib_recv.at[kind, g], sib_send.at[kind, g], sib_sem.at[kind, g], sibling)
    def mir_copy(g):
        return remote(comb.at[g], mir_recv.at[g], mir_send.at[g], mir_sem.at[g], mirror)

    def main_body():
        def q_cols(kind, g):
            if kind == 0:
                return jnp.concatenate([q_recv[1, g], q_recv[2, g]], axis=1)
            return jnp.concatenate([q_own[g], q_recv[0, g]], axis=1)

        def dot(a, b):
            return lax.dot_general(a, b, (((1,), (0,)), ((), ())), preferred_element_type=F32)

        def col_max(mx, s):
            return jnp.maximum(mx, jnp.max(s.reshape(s.shape[0] // 8, 8, 512), axis=0))

        def qk(q, g, kc, slot, mx):
            s = dot(kh[g, pl.ds(pl.multiple_of(kc * KEY_TILE, KEY_TILE), KEY_TILE), :], q)
            SB[slot][kc] = s
            return col_max(mx, s)

        def qk_new(q, kind, g, slot, mx):
            own, other = (me, sibling) if kind == 1 else (mirror, lax.rem(sibling + 2, 4))
            key = lax.broadcasted_iota(jnp.int32, (rows, 512), 0) + me * rows
            col = lax.broadcasted_iota(jnp.int32, (rows, 512), 1)
            row = lax.rem(col, rows) + jnp.where(col < 256, own, other) * rows
            s = jnp.where(key <= row, dot(k_new[g], q), -jnp.inf)
            sN[slot] = s
            return col_max(mx, s)

        def weights(s, mc, ls):
            p = jnp.exp2(s * SCALE_LOG2 - mc)
            return p.astype(BF16), ls + jnp.sum(p.reshape(s.shape[0] // 8, 8, 512), axis=0)

        def block(last, kind_n, g_n, g, b, par):
            steps = [("Q", i) for i in range(GROUP)] + [("Q", None)] * last
            for i in range(GROUP):
                steps.insert(LEAD + 2 * i, ("P", i))
            steps += [("P", None)] * last
            mx, ls, mc = mbuf[...], lbuf[...], mcb[0:1, :]
            q = q_cols(kind_n, g_n)
            acc = None
            for op, i in steps:
                if op == "Q" and i is None:
                    mx = qk_new(q, kind_n, g_n, 1 - par, mx)
                elif op == "Q":
                    mx = qk(q, g_n, b * GROUP + i, 1 - par, mx)
                else:
                    if i is None:
                        p, ls = weights(sN[par], mc, ls)
                        v = v_new[g]
                    else:
                        kc = b * GROUP + i
                        p, ls = weights(SB[par][kc], mc, ls)
                        v = vt[g, :, pl.ds(pl.multiple_of(kc * KEY_TILE, KEY_TILE), KEY_TILE)]
                    pv = dot(v, p)
                    acc = pv if acc is None else acc + pv
            mbuf[...] = mx
            lbuf[...] = ls
            if not last:
                obuf[...] += acc
                return None
            return obuf[...] + acc

        def merge(a, b):
            ma, mb = a[128:129, :], b[128:129, :]
            m = jnp.maximum(ma, mb)
            fa, fb = jnp.exp2(ma - m), jnp.exp2(mb - m)
            return a[0:128, :] * fa + b[0:128, :] * fb, m, a[129:130, :] * fa + b[129:130, :] * fb

        def unit(g, kind):
            par = kind
            if kind == 0:
                kind_n, g_n = 1, g
            else:
                kind_n, g_n = 0, jnp.minimum(g + 1, heads - 1)
            mcb[0:1, :] = jnp.max(mbuf[...], axis=0, keepdims=True) * SCALE_LOG2
            mbuf[...] = jnp.full(mbuf.shape, -jnp.inf, F32)
            lbuf[...] = jnp.zeros(lbuf.shape, F32)
            obuf[...] = jnp.zeros(obuf.shape, F32)
            nb = tiles // GROUP
            def ib(b, _):
                block(False, kind_n, g_n, g, b, par)
                return 0
            lax.fori_loop(0, nb - 1, ib, 0)
            acc = block(True, kind_n, g_n, g, nb - 1, par)
            for t in range(2):
                part[kind, g, t, 0:128, :] = acc[:, TS(t)]
                part[kind, g, t, 128:129, :] = mcb[0:1, TS(t)]
                part[kind, g, t, 129:130, :] = jnp.sum(lbuf[:, TS(t)], axis=0, keepdims=True)
            sib_copy(kind, g).start()
            if kind == 1:
                sib_copy(0, g).wait_recv()
                acc, m, total = merge(part.at[0, g, 0], sib_recv.at[0, g])
                comb[g, 0:128, :] = acc
                comb[g, 128:129, :] = m
                comb[g, 129:130, :] = total
                mir_copy(g).start()

        mbuf[...] = jnp.full(mbuf.shape, -jnp.inf, F32)
        q0 = q_cols(0, 0)
        def first(kc, _):
            mbuf[...] = qk(q0, 0, kc, 0, mbuf[...])
            return 0
        lax.fori_loop(0, tiles, first, 0)
        mbuf[...] = qk_new(q0, 0, 0, 0, mbuf[...])

        def body(g, _):
            unit(g, 0)
            unit(g, 1)
            return 0
        lax.fori_loop(0, heads, body, 0)

        def final(g, _):
            sib_copy(1, g).wait_recv()
            mir_copy(g).wait_recv()
            acc, m, total = merge(part.at[1, g, 0], sib_recv.at[1, g])
            mb = mir_recv[g, 128:129, :]
            top = jnp.maximum(m, mb)
            fa, fb = jnp.exp2(m - top), jnp.exp2(mb - top)
            acc = acc * fa + mir_recv[g, 0:128, :] * fb
            total = total * fa + mir_recv[g, 129:130, :] * fb
            o = acc / total
            for j in range(2):
                cols = pl.ds(pl.multiple_of((2 * g + j) * 128, 128), 128)
                att_ref[:, cols] = o[:, j * 128:(j + 1) * 128].T.astype(BF16)
            return 0
        lax.fori_loop(0, heads, final, 0)

    main_body()

    def drain(g, _):
        q_to_mirror(g).wait_send()
        q_to_sibling(g).wait_send()
        q_forward(g).wait_send()
        sib_copy(0, g).wait_send()
        sib_copy(1, g).wait_send()
        mir_copy(g).wait_send()
        return 0
    lax.fori_loop(0, heads, drain, 0)


def attend(q_own, k_new, v_new, k_cache, v_cache):
    n_keys, heads, _ = k_cache.shape
    rows = q_own.shape[2] // 2
    vm = pl.BlockSpec(memory_space=pltpu.VMEM)
    hbm = pl.BlockSpec(memory_space=pl.ANY)
    dma = pltpu.SemaphoreType.DMA
    tiles = n_keys // KEY_TILE
    return pl.pallas_call(
        functools.partial(attend_kernel, n_keys, heads),
        out_shape=jax.ShapeDtypeStruct((rows, 2 * heads * HEAD_DIM), BF16),
        in_specs=[vm, vm, vm, hbm, hbm],
        out_specs=vm,
        scratch_shapes=[
            pltpu.VMEM((heads, n_keys, 128), BF16), pltpu.VMEM((heads, 128, n_keys), BF16),
            pltpu.VMEM((tiles, KEY_TILE, 512), F32), pltpu.VMEM((tiles, KEY_TILE, 512), F32),
            pltpu.VMEM((2, rows, 512), F32),
            pltpu.VMEM((8, 512), F32), pltpu.VMEM((8, 512), F32), pltpu.VMEM((8, 512), F32), pltpu.VMEM((128, 512), F32),
            pltpu.VMEM((3, heads, 128, 256), BF16),
            pltpu.VMEM((2, heads, 2, 136, 256), F32), pltpu.VMEM((2, heads, 136, 256), F32),
            pltpu.VMEM((heads, 136, 256), F32), pltpu.VMEM((heads, 136, 256), F32),
            pltpu.VMEM((2, 2, PREP * heads, 128), BF16), pltpu.VMEM((2, PREP * heads, 128), F32),
            dma((2, 2)), dma((3, heads)), dma((3, heads)), dma((2, heads)), dma((2, heads)), dma((heads,)), dma((heads,)),
        ],
        compiler_params=pltpu.CompilerParams(vmem_limit_bytes=60 * 2**20, collective_id=0, has_side_effects=True),
    )(q_own, k_new, v_new, k_cache.reshape(n_keys * heads, 128), v_cache.reshape(n_keys * heads, 128))


def solution(mesh):
    cp_size = mesh.shape['cp']
    row_spec = P(('dp', 'cp'), None)
    cache_spec = P(('dp', 'cp'), None, None)
    whole = P()

    def device_step(x_rows, k_cache, v_cache, ln_gain, w_q, w_k, w_v, w_o, q_gain, k_gain):
        rows = x_rows.shape[0]
        prefix_len = k_cache.shape[0] * cp_size
        kv_heads = k_cache.shape[1]
        row_ids = lax.axis_index('cp') * rows + jnp.arange(rows)
        x_wide = x_rows.astype(F32)
        q_rot, k_new, v_new = project_rows(x_wide, ln_gain, w_q, w_k, w_v, q_gain, k_gain, prefix_len + row_ids)
        q_own = q_rot.reshape(rows, kv_heads, 2, HEAD_DIM).transpose(1, 3, 2, 0).reshape(kv_heads, HEAD_DIM, 2 * rows)
        att = attend(q_own, k_new.transpose(1, 0, 2), v_new.transpose(1, 2, 0), k_cache, v_cache)
        out = (x_wide + jnp.dot(att, w_o, preferred_element_type=F32)).astype(BF16)
        return out, k_new, v_new

    return jax.shard_map(device_step, mesh=mesh, in_specs=(row_spec, cache_spec, cache_spec, whole, whole, whole, whole, whole, whole, whole), out_specs=(row_spec, cache_spec, cache_spec), check_vma=False)
```

```python
import functools
import math

import jax
import jax.numpy as jnp
from jax import lax
from jax.experimental import pallas as pl
from jax.experimental.pallas import tpu as pltpu
from jax.sharding import PartitionSpec as P

HEAD_DIM = 128
ROPE_THETA = 1.0e6
NORM_EPS = 1.0e-6
SCALE_LOG2 = HEAD_DIM ** -0.5 * math.log2(math.e)
F32, BF16 = jnp.float32, jnp.bfloat16
MESH = pl.DeviceIdType.MESH

KEY_TILE = 256
PREP = 256
GROUP = 8
LEAD = 3


def rope_tables(positions):
    half = HEAD_DIM // 2
    inv_freq = ROPE_THETA ** (-jnp.arange(half, dtype=F32) * (2.0 / HEAD_DIM))
    angles = positions.astype(F32)[:, None] * inv_freq[None, :]
    cos_tab, sin_tab = jnp.cos(angles), jnp.sin(angles)
    return jnp.concatenate([cos_tab, cos_tab], axis=1), jnp.concatenate([-sin_tab, sin_tab], axis=1)


def block_kernel(n_keys, heads, x_ref, ln_gain, q_gain, k_gain, cos_tab, sin_tab, w_q, w_k, w_v, w_o, k_hbm, v_hbm,
                 out_ref, k_out, v_out,
                 hid, wbuf, att, q_own, k_new, v_new,
                 kh, vt, sA, sB, sN, mbuf, lbuf, mcb, obuf, q_recv, part, sib_recv, comb, mir_recv, raw, wide,
                 copy_sem, w_sem, q_send, q_sem, sib_send, sib_sem, mir_send, mir_sem):
    SB = (sA, sB)
    me = lax.axis_index("cp")
    sibling = me + 1 - 2 * lax.rem(me, 2)
    mirror = lax.rem(me + 2, 4)
    rows = 128
    tiles = n_keys // KEY_TILE
    units = 2 * heads
    TS = lambda t: slice(t * 256, (t + 1) * 256)

    def remote(src, dst, send, recv, to):
        return pltpu.make_async_remote_copy(src_ref=src, dst_ref=dst, send_sem=send, recv_sem=recv,
                                            device_id={"cp": to}, device_id_type=MESH)

    def cache_copy(i, which, slot):
        src = (k_hbm, v_hbm)[which]
        n = PREP * heads
        return pltpu.make_async_copy(src.at[pl.ds(pl.multiple_of(i * n, n), n), :], raw.at[which, slot], copy_sem.at[which, slot])

    WSLOTS = 4

    def weight_copy(w, c, slot):
        return pltpu.make_async_copy(w.at[:, pl.ds(pl.multiple_of(c * 256, 256), 256)], wbuf.at[slot], w_sem.at[slot])

    for c in range(WSLOTS):
        weight_copy(w_q, c, c).start()
    for s in range(2):
        cache_copy(s, 0, s).start()
        cache_copy(s, 1, s).start()

    xw = x_ref[...].astype(F32)
    mean_sq = jnp.mean(xw * xw, axis=-1, keepdims=True)
    hid[...] = (xw * lax.rsqrt(mean_sq + NORM_EPS) * ln_gain[...]).astype(BF16)

    barrier = pltpu.get_barrier_semaphore()
    for peer in (sibling, mirror):
        pl.semaphore_signal(barrier, inc=1, device_id={"cp": peer}, device_id_type=MESH)
    pl.semaphore_wait(barrier, 2)

    def q_to_sibling(g):
        return remote(q_own.at[g], q_recv.at[0, g], q_send.at[0, g], q_sem.at[0, g], sibling)
    def q_to_mirror(g):
        return remote(q_own.at[g], q_recv.at[1, g], q_send.at[1, g], q_sem.at[1, g], mirror)
    def q_forward(g):
        return remote(q_recv.at[1, g], q_recv.at[2, g], q_send.at[2, g], q_sem.at[2, g], sibling)
    def prep(i):
        slot = lax.rem(i, 2)
        row = pl.ds(pl.multiple_of(i * PREP, PREP), PREP)
        wide[0] = raw[0, slot].astype(F32)
        for h in range(heads):
            kh[h, row, :] = wide[0, pl.ds(h, PREP, stride=heads), :].astype(BF16)
        wide[1] = raw[1, slot].astype(F32)
        for h in range(heads):
            vt[h, :, row] = wide[1, pl.ds(h, PREP, stride=heads), :].T.astype(BF16)

    def head_rows(vals, gain):
        vals = vals.astype(BF16).astype(F32)
        normed = vals * lax.rsqrt(jnp.mean(vals * vals, axis=-1, keepdims=True) + NORM_EPS) * gain
        return normed * cos_tab[...] + pltpu.roll(normed, HEAD_DIM // 2, 1) * sin_tab[...]

    def load_step(i):
        wslot = lax.rem(i, WSLOTS)
        slot = lax.rem(i, 2)
        pltpu.make_async_copy(w_q.at[:, pl.ds(0, 256)], wbuf.at[wslot], w_sem.at[wslot]).wait()
        cache_copy(i, 0, slot).wait()
        cache_copy(i, 1, slot).wait()
        raw_cols = jnp.dot(hid[...], wbuf[wslot], preferred_element_type=F32)
        prep(i)
        return raw_cols

    def next_loads(i, w, c):
        if w is not None:
            weight_copy(w, c, lax.rem(i, WSLOTS)).start()
        @pl.when(i + 2 < n_keys // PREP)
        def _():
            cache_copy(i + 2, 0, lax.rem(i, 2)).start()
            cache_copy(i + 2, 1, lax.rem(i, 2)).start()

    n_q, n_kv = heads, heads // 2

    def q_step(i, w, c):
        cols = load_step(i)
        for j in range(2):
            r = head_rows(cols[:, j * 128:(j + 1) * 128], q_gain[...])
            q_own[i, :, j * 128:(j + 1) * 128] = r.T.astype(BF16)
        q_to_mirror(i).start()
        q_to_sibling(i).start()
        next_loads(i, w, c)

    def q_steps(lo, hi, w, off):
        def run(i, _):
            q_step(i, w, i - off)
            return 0
        lax.fori_loop(lo, hi, run, 0)
    q_steps(0, n_q - WSLOTS, w_q, -WSLOTS)
    q_steps(n_q - WSLOTS, n_q, w_k, n_q - WSLOTS)

    def k_step(c, _):
        cols = load_step(n_q + c)
        for j in range(2):
            r = head_rows(cols[:, j * 128:(j + 1) * 128], k_gain[...])
            k_new[2 * c + j] = r.astype(BF16)
        next_loads(n_q + c, w_v, c)
        return 0
    lax.fori_loop(0, n_kv, k_step, 0)

    def v_step(c, _):
        cols = load_step(n_q + n_kv + c)
        for j in range(2):
            v_new[2 * c + j] = cols[:, j * 128:(j + 1) * 128].T.astype(BF16)
        next_loads(n_q + n_kv + c, None, 0)
        return 0
    lax.fori_loop(0, n_kv, v_step, 0)
    for c in range(WSLOTS):
        weight_copy(w_o, c, c).start()

    for h in range(heads):
        wide[0, pl.ds(h, rows, stride=heads), :] = k_new[h].astype(F32)
        wide[1, pl.ds(h, rows, stride=heads), :] = v_new[h].astype(F32).T
    k_out[...] = wide[0, 0:rows * heads, :].astype(BF16)
    v_out[...] = wide[1, 0:rows * heads, :].astype(BF16)

    q_to_mirror(0).wait_recv()
    q_forward(0).start()
    q_to_sibling(0).wait_recv()
    q_forward(0).wait_recv()

    def sib_copy(kind, g):
        return remote(part.at[kind, g, 1], sib_recv.at[kind, g], sib_send.at[kind, g], sib_sem.at[kind, g], sibling)
    def mir_copy(g):
        return remote(comb.at[g], mir_recv.at[g], mir_send.at[g], mir_sem.at[g], mirror)

    def main_body():
        def q_cols(kind, g):
            if kind == 0:
                return jnp.concatenate([q_recv[1, g], q_recv[2, g]], axis=1)
            return jnp.concatenate([q_own[g], q_recv[0, g]], axis=1)

        def dot(a, b):
            return lax.dot_general(a, b, (((1,), (0,)), ((), ())), preferred_element_type=F32)

        def col_max(mx, s):
            return jnp.maximum(mx, jnp.max(s.reshape(s.shape[0] // 8, 8, 512), axis=0))

        def qk(q, g, kc, slot, mx):
            s = dot(kh[g, pl.ds(pl.multiple_of(kc * KEY_TILE, KEY_TILE), KEY_TILE), :], q)
            SB[slot][kc] = s
            return col_max(mx, s)

        def qk_new(q, kind, g, slot, mx):
            own, other = (me, sibling) if kind == 1 else (mirror, lax.rem(sibling + 2, 4))
            key = lax.broadcasted_iota(jnp.int32, (rows, 512), 0) + me * rows
            col = lax.broadcasted_iota(jnp.int32, (rows, 512), 1)
            row = lax.rem(col, rows) + jnp.where(col < 256, own, other) * rows
            s = jnp.where(key <= row, dot(k_new[g], q), -jnp.inf)
            sN[slot] = s
            return col_max(mx, s)

        def weights(s, mc, ls):
            p = jnp.exp2(s * SCALE_LOG2 - mc)
            return p.astype(BF16), ls + jnp.sum(p.reshape(s.shape[0] // 8, 8, 512), axis=0)

        def block(last, kind_n, g_n, g, b, par):
            steps = [("Q", i) for i in range(GROUP)] + [("Q", None)] * last
            for i in range(GROUP):
                steps.insert(LEAD + 2 * i, ("P", i))
            steps += [("P", None)] * last
            mx, ls, mc = mbuf[...], lbuf[...], mcb[par, 0:1, :]
            q = q_cols(kind_n, g_n)
            acc = None
            for op, i in steps:
                if op == "Q" and i is None:
                    mx = qk_new(q, kind_n, g_n, 1 - par, mx)
                elif op == "Q":
                    mx = qk(q, g_n, b * GROUP + i, 1 - par, mx)
                else:
                    if i is None:
                        p, ls = weights(sN[par], mc, ls)
                        v = v_new[g]
                    else:
                        kc = b * GROUP + i
                        p, ls = weights(SB[par][kc], mc, ls)
                        v = vt[g, :, pl.ds(pl.multiple_of(kc * KEY_TILE, KEY_TILE), KEY_TILE)]
                    pv = dot(v, p)
                    acc = pv if acc is None else acc + pv
            if not last:
                mbuf[...] = mx
                lbuf[...] = ls
                obuf[...] = acc
                return
            acc = obuf[...] + acc
            total = jnp.sum(ls, axis=0, keepdims=True)
            for t in range(2):
                part[par, g, t, 0:128, :] = acc[:, TS(t)]
                part[par, g, t, 128:129, :] = mc[:, TS(t)]
                part[par, g, t, 129:130, :] = total[:, TS(t)]
            mcb[1 - par, 0:1, :] = jnp.max(mx, axis=0, keepdims=True) * SCALE_LOG2
            mbuf[...] = jnp.full(mbuf.shape, -jnp.inf, F32)
            lbuf[...] = jnp.zeros(lbuf.shape, F32)

        def merge(a, b):
            ma, mb = a[128:129, :], b[128:129, :]
            m = jnp.maximum(ma, mb)
            fa, fb = jnp.exp2(ma - m), jnp.exp2(mb - m)
            return a[0:128, :] * fa + b[0:128, :] * fb, m, a[129:130, :] * fa + b[129:130, :] * fb

        def unit(g, kind):
            kind_n, g_n = (1, g) if kind == 0 else (0, jnp.minimum(g + 1, heads - 1))
            @pl.when(g < 2 * heads)
            def _():
                block(False, kind_n, g_n, g, 0, kind)
            if kind == 1:
                sib_copy(0, g).wait_recv()
                acc, m, total = merge(part.at[0, g, 0], sib_recv.at[0, g])
                comb[g, 0:128, :] = acc
                comb[g, 128:129, :] = m
                comb[g, 129:130, :] = total
                mir_copy(g).start()
            @pl.when(g < 3 * heads)
            def _():
                block(True, kind_n, g_n, g, 1, kind)
            sib_copy(kind, g).start()

        mbuf[...] = jnp.full(mbuf.shape, -jnp.inf, F32)
        q0 = q_cols(0, 0)
        def first(b, _):
            mx = mbuf[...]
            for c in range(4):
                mx = qk(q0, 0, 4 * b + c, 0, mx)
            mbuf[...] = mx
            return 0
        lax.fori_loop(0, tiles // 4, first, 0)
        mx = qk_new(q0, 0, 0, 0, mbuf[...])
        mcb[0, 0:1, :] = jnp.max(mx, axis=0, keepdims=True) * SCALE_LOG2
        mbuf[...] = jnp.full(mbuf.shape, -jnp.inf, F32)
        lbuf[...] = jnp.zeros(lbuf.shape, F32)

        def body(g, _):
            @pl.when(g + 1 < heads)
            def _():
                q_to_mirror(g + 1).wait_recv()
                q_forward(g + 1).start()
            unit(g, 0)
            @pl.when(g + 1 < heads)
            def _():
                q_to_sibling(g + 1).wait_recv()
                q_forward(g + 1).wait_recv()
            unit(g, 1)
            return 0
        lax.fori_loop(0, heads, body, 0)

        def final(g, _):
            sib_copy(1, g).wait_recv()
            mir_copy(g).wait_recv()
            acc, m, total = merge(part.at[1, g, 0], sib_recv.at[1, g])
            mb = mir_recv[g, 128:129, :]
            top = jnp.maximum(m, mb)
            fa, fb = jnp.exp2(m - top), jnp.exp2(mb - top)
            acc = acc * fa + mir_recv[g, 0:128, :] * fb
            total = total * fa + mir_recv[g, 129:130, :] * fb
            o = acc / total
            for j in range(2):
                cols = pl.ds(pl.multiple_of((2 * g + j) * 128, 128), 128)
                att[:, cols] = o[:, j * 128:(j + 1) * 128].T.astype(BF16)
            return 0
        lax.fori_loop(0, heads, final, 0)
        n_out = x_ref.shape[1] // 256
        def project(n, _):
            slot = lax.rem(n, WSLOTS)
            weight_copy(w_o, n, slot).wait()
            cols = pl.ds(pl.multiple_of(n * 256, 256), 256)
            add = jnp.dot(att[...], wbuf[slot], preferred_element_type=F32)
            out_ref[:, cols] = (x_ref[:, cols].astype(F32) + add).astype(BF16)
            @pl.when(n + WSLOTS < n_out)
            def _():
                weight_copy(w_o, n + WSLOTS, slot).start()
            return 0
        lax.fori_loop(0, n_out, project, 0)

    main_body()

    def drain(g, _):
        q_to_mirror(g).wait_send()
        q_to_sibling(g).wait_send()
        q_forward(g).wait_send()
        sib_copy(0, g).wait_send()
        sib_copy(1, g).wait_send()
        mir_copy(g).wait_send()
        return 0
    lax.fori_loop(0, heads, drain, 0)


def attention_block(x, ln_gain, q_gain, k_gain, cos_tab, sin_tab, w_q, w_k, w_v, w_o, k_cache, v_cache):
    n_keys, heads, _ = k_cache.shape
    rows, width = x.shape
    vm = pl.BlockSpec(memory_space=pltpu.VMEM)
    hbm = pl.BlockSpec(memory_space=pl.ANY)
    dma = pltpu.SemaphoreType.DMA
    tiles = n_keys // KEY_TILE
    return pl.pallas_call(
        functools.partial(block_kernel, n_keys, heads),
        out_shape=(jax.ShapeDtypeStruct((rows, width), BF16), jax.ShapeDtypeStruct((rows * heads, HEAD_DIM), BF16),
                   jax.ShapeDtypeStruct((rows * heads, HEAD_DIM), BF16)),
        in_specs=[vm] * 6 + [hbm] * 6,
        out_specs=(vm, vm, vm),
        scratch_shapes=[
            pltpu.VMEM((rows, width), BF16), pltpu.VMEM((4, width, 256), BF16),
            pltpu.VMEM((rows, w_o.shape[0]), BF16), pltpu.VMEM((heads, 128, 256), BF16),
            pltpu.VMEM((heads, rows, 128), BF16), pltpu.VMEM((heads, 128, rows), BF16),
            pltpu.VMEM((heads, n_keys, 128), BF16), pltpu.VMEM((heads, 128, n_keys), BF16),
            pltpu.VMEM((tiles, KEY_TILE, 512), F32), pltpu.VMEM((tiles, KEY_TILE, 512), F32),
            pltpu.VMEM((2, rows, 512), F32),
            pltpu.VMEM((8, 512), F32), pltpu.VMEM((8, 512), F32), pltpu.VMEM((2, 8, 512), F32), pltpu.VMEM((128, 512), F32),
            pltpu.VMEM((3, heads, 128, 256), BF16),
            pltpu.VMEM((2, heads, 2, 136, 256), F32), pltpu.VMEM((2, heads, 136, 256), F32),
            pltpu.VMEM((heads, 136, 256), F32), pltpu.VMEM((heads, 136, 256), F32),
            pltpu.VMEM((2, 2, PREP * heads, 128), BF16), pltpu.VMEM((2, PREP * heads, 128), F32),
            dma((2, 2)), dma((4,)), dma((3, heads)), dma((3, heads)), dma((2, heads)), dma((2, heads)), dma((heads,)), dma((heads,)),
        ],
        compiler_params=pltpu.CompilerParams(vmem_limit_bytes=67043328, collective_id=0, has_side_effects=True),
    )(x, ln_gain, q_gain, k_gain, cos_tab, sin_tab, w_q, w_k, w_v, w_o,
      k_cache.reshape(n_keys * heads, HEAD_DIM), v_cache.reshape(n_keys * heads, HEAD_DIM))


def solution(mesh):
    cp_size = mesh.shape['cp']
    row_spec = P(('dp', 'cp'), None)
    cache_spec = P(('dp', 'cp'), None, None)
    whole = P()

    def device_step(x_rows, k_cache, v_cache, ln_gain, w_q, w_k, w_v, w_o, q_gain, k_gain):
        rows = x_rows.shape[0]
        n_keys, heads, _ = k_cache.shape
        positions = n_keys * cp_size + lax.axis_index('cp') * rows + jnp.arange(rows)
        cos_tab, sin_tab = rope_tables(positions)
        wide_row = lambda v: v.astype(F32)[None, :]
        out, k_new, v_new = attention_block(x_rows, wide_row(ln_gain), wide_row(q_gain), wide_row(k_gain), cos_tab, sin_tab,
                                            w_q, w_k, w_v, w_o, k_cache, v_cache)
        return out, k_new.reshape(rows, heads, HEAD_DIM), v_new.reshape(rows, heads, HEAD_DIM)

    return jax.shard_map(device_step, mesh=mesh, in_specs=(row_spec, cache_spec, cache_spec, whole, whole, whole, whole, whole, whole, whole), out_specs=(row_spec, cache_spec, cache_spec), check_vma=False)
```

```python
import functools
import math

import jax
import jax.numpy as jnp
from jax import lax
from jax.experimental import pallas as pl
from jax.experimental.pallas import tpu as pltpu
from jax.sharding import PartitionSpec as P

HEAD_DIM = 128
ROPE_THETA = 1.0e6
NORM_EPS = 1.0e-6
SCALE_LOG2 = HEAD_DIM ** -0.5 * math.log2(math.e)
F32, BF16 = jnp.float32, jnp.bfloat16
MESH = pl.DeviceIdType.MESH

KEY_TILE = 256
PREP = 256
GROUP = 16
LEAD = 1


def rope_tables(positions):
    half = HEAD_DIM // 2
    inv_freq = ROPE_THETA ** (-jnp.arange(half, dtype=F32) * (2.0 / HEAD_DIM))
    angles = positions.astype(F32)[:, None] * inv_freq[None, :]
    return jnp.cos(angles), jnp.sin(angles)


def block_kernel(n_keys, heads, x_ref, ln_gain, q_gain, k_gain, cos_tab, sin_tab, w_q, w_k, w_v, w_o, k_hbm, v_hbm,
                 out_ref, k_out, v_out,
                 hid, wbuf, cols, cosw, sinw, att, k_new, v_new,
                 kh, vt, sA, sB, sN, mbuf, lbuf, mcb, obuf, qs, part, sib_recv, comb, mir_recv, raw, wide,
                 copy_sem, w_sem, q_send, q_sem, sib_send, sib_sem, mir_send, mir_sem):
    SB = (sA, sB)
    me = lax.axis_index("cp")
    sibling = me + 1 - 2 * lax.rem(me, 2)
    mirror = lax.rem(me + 2, 4)
    rows = 128
    tiles = n_keys // KEY_TILE
    units = 2 * heads
    TS = lambda t: slice(t * 256, (t + 1) * 256)

    def remote(src, dst, send, recv, to):
        return pltpu.make_async_remote_copy(src_ref=src, dst_ref=dst, send_sem=send, recv_sem=recv,
                                            device_id={"cp": to}, device_id_type=MESH)

    def cache_copy(i, which, slot):
        src = (k_hbm, v_hbm)[which]
        n = PREP * heads
        return pltpu.make_async_copy(src.at[pl.ds(pl.multiple_of(i * n, n), n), :], raw.at[which, slot], copy_sem.at[which, slot])

    WSLOTS = 4

    def weight_copy(w, c, slot):
        return pltpu.make_async_copy(w.at[:, pl.ds(pl.multiple_of(c * 256, 256), 256)], wbuf.at[slot], w_sem.at[slot])

    for c in range(WSLOTS):
        weight_copy(w_q, c, c).start()
    for s in range(2):
        cache_copy(s, 0, s).start()
        cache_copy(s, 1, s).start()

    xw = x_ref[...].astype(F32)
    mean_sq = jnp.mean(xw * xw, axis=-1, keepdims=True)
    hid[...] = (xw * lax.rsqrt(mean_sq + NORM_EPS) * ln_gain[...].astype(F32).reshape(1, -1)).astype(BF16)
    cosw[...] = jnp.concatenate([cos_tab[...], cos_tab[...]], axis=1)
    sinw[...] = jnp.concatenate([-sin_tab[...], sin_tab[...]], axis=1)

    barrier = pltpu.get_barrier_semaphore()
    for peer in (sibling, mirror):
        pl.semaphore_signal(barrier, inc=1, device_id={"cp": peer}, device_id_type=MESH)
    pl.semaphore_wait(barrier, 2)

    def q_to_sibling(g):
        return remote(qs.at[0, g], qs.at[1, g], q_send.at[0, g], q_sem.at[0, g], sibling)
    def q_to_mirror(g):
        return remote(qs.at[0, g], qs.at[2, g], q_send.at[1, g], q_sem.at[1, g], mirror)
    def q_forward(g):
        return remote(qs.at[2, g], qs.at[3, g], q_send.at[2, g], q_sem.at[2, g], sibling)

    def prep(i):
        slot = lax.rem(i, 2)
        row = pl.ds(pl.multiple_of(i * PREP, PREP), PREP)
        wide[0] = raw[0, slot].astype(F32)
        for h in range(heads):
            kh[h, row, :] = wide[0, pl.ds(h, PREP, stride=heads), :].astype(BF16)
        wide[1] = raw[1, slot].astype(F32)
        for h in range(heads):
            vt[h, :, row] = wide[1, pl.ds(h, PREP, stride=heads), :].T.astype(BF16)

    def head_rows(vals, gain):
        vals = vals.astype(BF16).astype(F32)
        normed = vals * lax.rsqrt(jnp.mean(vals * vals, axis=-1, keepdims=True) + NORM_EPS) * gain
        return normed * cosw[...] + pltpu.roll(normed, HEAD_DIM // 2, 1) * sinw[...]

    n_q, n_kv = heads, heads // 2
    steps = n_q + 2 * n_kv

    def load_step(i, post):
        wslot = lax.rem(i, WSLOTS)
        slot = lax.rem(i, 2)
        weight_copy(w_q, 0, wslot).wait()
        cache_copy(i, 0, slot).wait()
        cache_copy(i, 1, slot).wait()
        done = cols[...]
        fresh = jnp.dot(hid[...], wbuf[wslot], preferred_element_type=F32)
        prep(i)
        post(i - 1, done)
        cols[...] = fresh
        ahead = i + WSLOTS
        for w, lo, hi in ((w_q, 0, n_q), (w_k, n_q, n_q + n_kv), (w_v, n_q + n_kv, steps), (w_o, steps, steps + WSLOTS)):
            @pl.when((ahead >= lo) & (ahead < hi))
            def _():
                weight_copy(w, ahead - lo, wslot).start()
        @pl.when(i + 2 < n_keys // PREP)
        def _():
            cache_copy(i + 2, 0, slot).start()
            cache_copy(i + 2, 1, slot).start()

    def halves(vals):
        return [vals[:, j * 128:(j + 1) * 128] for j in range(2)]

    def q_post(g, vals):
        for j, half in enumerate(halves(vals)):
            qs[0, g, :, j * 128:(j + 1) * 128] = head_rows(half, q_gain[...].astype(F32).reshape(1, -1)).T.astype(BF16)

    def k_post(c, vals):
        for j, half in enumerate(halves(vals)):
            k_new[2 * (c - n_q) + j] = head_rows(half, k_gain[...].astype(F32).reshape(1, -1)).astype(BF16)

    def v_post(c, vals):
        for j, half in enumerate(halves(vals)):
            v_new[2 * (c - n_q - n_kv) + j] = half.T.astype(BF16)

    load_step(0, lambda i, vals: None)

    def q_steps(i, _):
        load_step(i, q_post)
        q_to_mirror(i - 1).start()
        q_to_sibling(i - 1).start()
        return 0
    lax.fori_loop(1, n_q + 1, q_steps, 0)

    def k_steps(i, _):
        load_step(i, k_post)
        return 0
    lax.fori_loop(n_q + 1, n_q + n_kv + 1, k_steps, 0)

    def v_steps(i, _):
        load_step(i, v_post)
        return 0
    lax.fori_loop(n_q + n_kv + 1, steps, v_steps, 0)
    v_post(steps - 1, cols[...])

    for h in range(heads):
        wide[0, pl.ds(h, rows, stride=heads), :] = k_new[h].astype(F32)
        wide[1, pl.ds(h, rows, stride=heads), :] = v_new[h].astype(F32).T
    k_out[...] = wide[0, 0:rows * heads, :].astype(BF16)
    v_out[...] = wide[1, 0:rows * heads, :].astype(BF16)

    for g in range(2):
        q_to_mirror(g).wait_recv()
        q_forward(g).start()
    q_to_sibling(0).wait_recv()
    q_forward(0).wait_recv()

    def sib_copy(kind, g):
        return remote(part.at[kind, g, 1], sib_recv.at[kind, g], sib_send.at[kind, g], sib_sem.at[kind, g], sibling)
    def mir_copy(g):
        return remote(comb.at[g], mir_recv.at[g], mir_send.at[g], mir_sem.at[g], mirror)

    def main_body():
        def q_cols(kind, g):
            base = 2 - 2 * kind
            return jnp.concatenate([qs[base, g], qs[base + 1, g]], axis=1)

        def dot(a, b):
            return lax.dot_general(a, b, (((1,), (0,)), ((), ())), preferred_element_type=F32)

        def col_max(mx, s):
            return jnp.maximum(mx, jnp.max(s.reshape(s.shape[0] // 8, 8, 512), axis=0))

        def qk(q, g, kc, slot, mx):
            s = dot(kh[g, pl.ds(pl.multiple_of(kc * KEY_TILE, KEY_TILE), KEY_TILE), :], q)
            SB[slot][kc] = s
            return col_max(mx, s)

        def qk_new(q, kind, g, slot, mx):
            own = lax.rem(me + 2 * (1 - kind), 4)
            other = lax.rem(sibling + 2 * (1 - kind), 4)
            key = lax.broadcasted_iota(jnp.int32, (rows, 512), 0) + me * rows
            col = lax.broadcasted_iota(jnp.int32, (rows, 512), 1)
            row = lax.rem(col, rows) + jnp.where(col < 256, own, other) * rows
            s = jnp.where(key <= row, dot(k_new[g], q), -jnp.inf)
            sN[slot] = s
            return col_max(mx, s)

        def weights(s, mc, ls):
            p = jnp.exp2(s * SCALE_LOG2 - mc)
            return p.astype(BF16), ls + jnp.sum(p.reshape(s.shape[0] // 8, 8, 512), axis=0)

        def block(last, kind_n, g_n, kind, g, b, par):
            steps = [("Q", i) for i in range(GROUP)] + [("Q", None)] * last
            for i in range(GROUP):
                steps.insert(LEAD + 2 * i, ("P", i))
            steps += [("P", None)] * last
            mx, ls, mc = mbuf[...], lbuf[...], mcb[par, 0:1, :]
            q = q_cols(kind_n, g_n)
            acc = None
            for op, i in steps:
                if op == "Q" and i is None:
                    mx = qk_new(q, kind_n, g_n, 1 - par, mx)
                elif op == "Q":
                    mx = qk(q, g_n, b * GROUP + i, 1 - par, mx)
                else:
                    if i is None:
                        p, ls = weights(sN[par], mc, ls)
                        v = v_new[g]
                    else:
                        kc = b * GROUP + i
                        p, ls = weights(SB[par][kc], mc, ls)
                        v = vt[g, :, pl.ds(pl.multiple_of(kc * KEY_TILE, KEY_TILE), KEY_TILE)]
                    pv = dot(v, p)
                    acc = pv if acc is None else acc + pv
            if not last:
                mbuf[...] = mx
                lbuf[...] = ls
                obuf[...] = acc
                return
            acc = obuf[...] + acc
            total = jnp.sum(ls, axis=0, keepdims=True)
            for t in range(2):
                part[kind, g, t, 0:128, :] = acc[:, TS(t)]
                part[kind, g, t, 128:129, :] = mc[:, TS(t)]
                part[kind, g, t, 129:130, :] = total[:, TS(t)]
            mcb[1 - par, 0:1, :] = jnp.max(mx, axis=0, keepdims=True) * SCALE_LOG2
            mbuf[...] = jnp.full(mbuf.shape, -jnp.inf, F32)
            lbuf[...] = jnp.zeros(lbuf.shape, F32)

        def merge(a, b):
            ma, mb = a[128:129, :], b[128:129, :]
            m = jnp.maximum(ma, mb)
            fa, fb = jnp.exp2(ma - m), jnp.exp2(mb - m)
            return a[0:128, :] * fa + b[0:128, :] * fb, m, a[129:130, :] * fa + b[129:130, :] * fb

        def send_merged(g):
            sib_copy(0, g).wait_recv()
            acc, m, total = merge(part.at[0, g, 0], sib_recv.at[0, g])
            comb[g, 0:128, :] = acc
            comb[g, 128:129, :] = m
            comb[g, 129:130, :] = total
            mir_copy(g).start()

        def unit_of(pos):
            half = pos // 2
            odd = pos - 2 * half
            local = jnp.where((odd == 0) & (half > 0) | (pos >= 2 * heads - 1), 1, 0)
            return local, jnp.where(pos >= 2 * heads - 1, heads - 1, jnp.maximum(half - 1 + 2 * odd, 0))

        def unit(p, par):
            pos = 2 * p + par
            kind, g = unit_of(pos)
            kind_n, g_n = unit_of(jnp.minimum(pos + 1, 2 * heads - 1))
            for b in range(tiles // GROUP):
                @pl.when(p < (2 + b) * heads)
                def _():
                    block(b == tiles // GROUP - 1, kind_n, g_n, kind, g, b, par)
                if b == 0:
                    @pl.when((p == 0) if par else (p > 0))
                    def _():
                        send_merged(p)
            sib_copy(kind, g).start()

        mbuf[...] = jnp.full(mbuf.shape, -jnp.inf, F32)
        q0 = q_cols(0, 0)
        def first(b, _):
            mx = mbuf[...]
            for c in range(4):
                mx = qk(q0, 0, 4 * b + c, 0, mx)
            mbuf[...] = mx
            return 0
        lax.fori_loop(0, tiles // 4, first, 0)
        mx = qk_new(q0, 0, 0, 0, mbuf[...])
        mcb[0, 0:1, :] = jnp.max(mx, axis=0, keepdims=True) * SCALE_LOG2
        mbuf[...] = jnp.full(mbuf.shape, -jnp.inf, F32)
        lbuf[...] = jnp.zeros(lbuf.shape, F32)

        def body(p, _):
            @pl.when(p + 1 < heads)
            def _():
                q_to_sibling(p + 1).wait_recv()
                q_forward(p + 1).wait_recv()
            unit(p, 0)
            @pl.when(p + 2 < heads)
            def _():
                q_to_mirror(p + 2).wait_recv()
                q_forward(p + 2).start()
            unit(p, 1)
            return 0
        lax.fori_loop(0, heads, body, 0)

        def final(g, _):
            sib_copy(1, g).wait_recv()
            mir_copy(g).wait_recv()
            acc, m, total = merge(part.at[1, g, 0], sib_recv.at[1, g])
            mb = mir_recv[g, 128:129, :]
            top = jnp.maximum(m, mb)
            fa, fb = jnp.exp2(m - top), jnp.exp2(mb - top)
            acc = acc * fa + mir_recv[g, 0:128, :] * fb
            total = total * fa + mir_recv[g, 129:130, :] * fb
            o = acc / total
            for j in range(2):
                cols = pl.ds(pl.multiple_of((2 * g + j) * 128, 128), 128)
                att[:, cols] = o[:, j * 128:(j + 1) * 128].T.astype(BF16)
            return 0
        lax.fori_loop(0, heads, final, 0)
        n_out = x_ref.shape[1] // 256
        def project(n, _):
            slot = lax.rem(n, WSLOTS)
            weight_copy(w_o, n, slot).wait()
            cols = pl.ds(pl.multiple_of(n * 256, 256), 256)
            add = jnp.dot(att[...], wbuf[slot], preferred_element_type=F32)
            out_ref[:, cols] = (x_ref[:, cols].astype(F32) + add).astype(BF16)
            @pl.when(n + WSLOTS < n_out)
            def _():
                weight_copy(w_o, n + WSLOTS, slot).start()
            return 0
        lax.fori_loop(0, n_out, project, 0)

    main_body()

    def drain(g, _):
        q_to_mirror(g).wait_send()
        q_to_sibling(g).wait_send()
        q_forward(g).wait_send()
        sib_copy(0, g).wait_send()
        sib_copy(1, g).wait_send()
        mir_copy(g).wait_send()
        return 0
    lax.fori_loop(0, heads, drain, 0)


def attention_block(x, ln_gain, q_gain, k_gain, cos_tab, sin_tab, w_q, w_k, w_v, w_o, k_cache, v_cache):
    n_keys, heads, _ = k_cache.shape
    rows, width = x.shape
    vm = pl.BlockSpec(memory_space=pltpu.VMEM)
    hbm = pl.BlockSpec(memory_space=pl.ANY)
    dma = pltpu.SemaphoreType.DMA
    tiles = n_keys // KEY_TILE
    return pl.pallas_call(
        functools.partial(block_kernel, n_keys, heads),
        out_shape=(jax.ShapeDtypeStruct((rows, width), BF16), jax.ShapeDtypeStruct((rows * heads, HEAD_DIM), BF16),
                   jax.ShapeDtypeStruct((rows * heads, HEAD_DIM), BF16)),
        in_specs=[vm] * 6 + [hbm] * 6,
        out_specs=(vm, vm, vm),
        scratch_shapes=[
            pltpu.VMEM((rows, width), BF16), pltpu.VMEM((4, width, 256), BF16),
            pltpu.VMEM((rows, 256), F32), pltpu.VMEM((rows, 128), F32), pltpu.VMEM((rows, 128), F32), pltpu.VMEM((rows, w_o.shape[0]), BF16),
            pltpu.VMEM((heads, rows, 128), BF16), pltpu.VMEM((heads, 128, rows), BF16),
            pltpu.VMEM((heads, n_keys, 128), BF16), pltpu.VMEM((heads, 128, n_keys), BF16),
            pltpu.VMEM((tiles, KEY_TILE, 512), F32), pltpu.VMEM((tiles, KEY_TILE, 512), F32),
            pltpu.VMEM((2, rows, 512), F32),
            pltpu.VMEM((8, 512), F32), pltpu.VMEM((8, 512), F32), pltpu.VMEM((2, 8, 512), F32), pltpu.VMEM((128, 512), F32),
            pltpu.VMEM((4, heads, 128, 256), BF16),
            pltpu.VMEM((2, heads, 2, 136, 256), F32), pltpu.VMEM((2, heads, 136, 256), F32),
            pltpu.VMEM((heads, 136, 256), F32), pltpu.VMEM((heads, 136, 256), F32),
            pltpu.VMEM((2, 2, PREP * heads, 128), BF16), pltpu.VMEM((2, PREP * heads, 128), F32),
            dma((2, 2)), dma((4,)), dma((3, heads)), dma((3, heads)), dma((2, heads)), dma((2, heads)), dma((heads,)), dma((heads,)),
        ],
        compiler_params=pltpu.CompilerParams(vmem_limit_bytes=62 * 2**20, collective_id=0, has_side_effects=True),
    )(x, ln_gain, q_gain, k_gain, cos_tab, sin_tab, w_q, w_k, w_v, w_o,
      k_cache.reshape(n_keys * heads, HEAD_DIM), v_cache.reshape(n_keys * heads, HEAD_DIM))


def pass_on(*arrays):
    def kernel(*refs):
        n = len(refs) // 2
        for src, dst in zip(refs[:n], refs[n:]):
            dst[...] = src[...]
    vm = pl.BlockSpec(memory_space=pltpu.VMEM)
    return pl.pallas_call(kernel, out_shape=tuple(jax.ShapeDtypeStruct(a.shape, a.dtype) for a in arrays),
                          in_specs=[vm] * len(arrays), out_specs=(vm,) * len(arrays))(*arrays)


def solution(mesh):
    cp_size = mesh.shape['cp']
    row_spec = P(('dp', 'cp'), None)
    cache_spec = P(('dp', 'cp'), None, None)
    whole = P()

    def device_step(x_rows, k_cache, v_cache, ln_gain, w_q, w_k, w_v, w_o, q_gain, k_gain):
        rows = x_rows.shape[0]
        n_keys, heads, _ = k_cache.shape
        positions = n_keys * cp_size + lax.axis_index('cp') * rows + jnp.arange(rows)
        cos_tab, sin_tab = rope_tables(positions)
        out, k_new, v_new = pass_on(*attention_block(x_rows, ln_gain, q_gain, k_gain, cos_tab, sin_tab, w_q, w_k, w_v, w_o, k_cache, v_cache))
        return out, k_new.reshape(rows, heads, HEAD_DIM), v_new.reshape(rows, heads, HEAD_DIM)

    return jax.shard_map(device_step, mesh=mesh, in_specs=(row_spec, cache_spec, cache_spec, whole, whole, whole, whole, whole, whole, whole), out_specs=(row_spec, cache_spec, cache_spec), check_vma=False)
```

```python
import functools
import math

import jax
import jax.numpy as jnp
from jax import lax
from jax.experimental import pallas as pl
from jax.experimental.pallas import tpu as pltpu
from jax.sharding import PartitionSpec as P

HEAD_DIM = 128
ROPE_THETA = 1.0e6
NORM_EPS = 1.0e-6
SCALE_LOG2 = HEAD_DIM ** -0.5 * math.log2(math.e)
F32, BF16 = jnp.float32, jnp.bfloat16
MESH = pl.DeviceIdType.MESH

KEY_TILE = 256
PREP = 256
GROUP = 16
WSLOTS = 4
CSLOTS = 4
LEAD = 1


def rope_tables(positions):
    half = HEAD_DIM // 2
    inv_freq = ROPE_THETA ** (-jnp.arange(half, dtype=F32) * (2.0 / HEAD_DIM))
    angles = positions.astype(F32)[:, None] * inv_freq[None, :]
    return jnp.cos(angles), jnp.sin(angles)


def block_kernel(n_keys, heads, x_ref, ln_gain, q_gain, k_gain, cos_tab, sin_tab, w_q, w_k, w_v, w_o, k_hbm, v_hbm,
                 out_ref, k_out, v_out,
                 hid, wbuf, cols, cosw, sinw, att, k_new, v_new,
                 kh, vt, sA, sB, sN, mbuf, lbuf, mcb, obuf, qs, part, sib_recv, comb, mir_recv, raw, wide,
                 copy_sem, w_sem, q_send, q_sem, sib_send, sib_sem, mir_send, mir_sem):
    SB = (sA, sB)
    me = lax.axis_index("cp")
    sibling = me + 1 - 2 * lax.rem(me, 2)
    mirror = lax.rem(me + 2, 4)
    rows = 128
    tiles = n_keys // KEY_TILE
    units = 2 * heads
    TS = lambda t: slice(t * 256, (t + 1) * 256)

    def remote(src, dst, send, recv, to):
        return pltpu.make_async_remote_copy(src_ref=src, dst_ref=dst, send_sem=send, recv_sem=recv,
                                            device_id={"cp": to}, device_id_type=MESH)

    def cache_copy(i, which, slot):
        src = (k_hbm, v_hbm)[which]
        n = PREP * heads
        return pltpu.make_async_copy(src.at[pl.ds(pl.multiple_of(i * n, n), n), :], raw.at[which, slot], copy_sem.at[which, slot])

    def weight_copy(w, c, slot):
        return pltpu.make_async_copy(w.at[:, pl.ds(pl.multiple_of(c * 256, 256), 256)], wbuf.at[slot], w_sem.at[slot])

    for c in range(WSLOTS):
        weight_copy(w_q, c, c).start()
    for s in range(CSLOTS):
        cache_copy(s, 0, s).start()
        cache_copy(s, 1, s).start()

    xw = x_ref[...].astype(F32)
    mean_sq = jnp.mean(xw * xw, axis=-1, keepdims=True)
    hid[...] = (xw * lax.rsqrt(mean_sq + NORM_EPS) * ln_gain[...].astype(F32).reshape(1, -1)).astype(BF16)
    cosw[...] = jnp.concatenate([cos_tab[...], cos_tab[...]], axis=1)
    sinw[...] = jnp.concatenate([-sin_tab[...], sin_tab[...]], axis=1)

    barrier = pltpu.get_barrier_semaphore()
    for peer in (sibling, mirror):
        pl.semaphore_signal(barrier, inc=1, device_id={"cp": peer}, device_id_type=MESH)
    pl.semaphore_wait(barrier, 2)

    def q_to_sibling(g):
        return remote(qs.at[0, g], qs.at[1, g], q_send.at[0, g], q_sem.at[0, g], sibling)
    def q_to_mirror(g):
        return remote(qs.at[0, g], qs.at[2, g], q_send.at[1, g], q_sem.at[1, g], mirror)
    def q_forward(g):
        return remote(qs.at[2, g], qs.at[3, g], q_send.at[2, g], q_sem.at[2, g], sibling)

    def prep(i):
        slot = lax.rem(i, CSLOTS)
        row = pl.ds(pl.multiple_of(i * PREP, PREP), PREP)
        wide[0] = raw[0, slot].astype(F32)
        for h in range(heads):
            kh[h, row, :] = wide[0, pl.ds(h, PREP, stride=heads), :].astype(BF16)
        wide[1] = raw[1, slot].astype(F32)
        for h in range(heads):
            vt[h, :, row] = wide[1, pl.ds(h, PREP, stride=heads), :].T.astype(BF16)

    def head_rows(vals, gain):
        vals = vals.astype(BF16).astype(F32)
        normed = vals * lax.rsqrt(jnp.mean(vals * vals, axis=-1, keepdims=True) + NORM_EPS) * gain
        return normed * cosw[...] + pltpu.roll(normed, HEAD_DIM // 2, 1) * sinw[...]

    n_q, n_kv = heads, heads // 2
    steps = n_q + 2 * n_kv

    def load_step(i, post):
        wslot = lax.rem(i, WSLOTS)
        slot = lax.rem(i, CSLOTS)
        weight_copy(w_q, 0, wslot).wait()
        cache_copy(i, 0, slot).wait()
        cache_copy(i, 1, slot).wait()
        done = cols[...]
        fresh = jnp.dot(hid[...], wbuf[wslot], preferred_element_type=F32)
        prep(i)
        post(i - 1, done)
        cols[...] = fresh
        ahead = i + WSLOTS
        for w, lo, hi in ((w_q, 0, n_q), (w_k, n_q, n_q + n_kv), (w_v, n_q + n_kv, steps), (w_o, steps, steps + WSLOTS)):
            @pl.when((ahead >= lo) & (ahead < hi))
            def _():
                weight_copy(w, ahead - lo, wslot).start()
        @pl.when(i + CSLOTS < n_keys // PREP)
        def _():
            cache_copy(i + CSLOTS, 0, slot).start()
            cache_copy(i + CSLOTS, 1, slot).start()

    def halves(vals):
        return [vals[:, j * 128:(j + 1) * 128] for j in range(2)]

    def q_post(g, vals):
        for j, half in enumerate(halves(vals)):
            qs[0, g, :, j * 128:(j + 1) * 128] = head_rows(half, q_gain[...].astype(F32).reshape(1, -1)).T.astype(BF16)

    def k_post(c, vals):
        for j, half in enumerate(halves(vals)):
            k_new[2 * (c - n_q) + j] = head_rows(half, k_gain[...].astype(F32).reshape(1, -1)).astype(BF16)

    def v_post(c, vals):
        for j, half in enumerate(halves(vals)):
            v_new[2 * (c - n_q - n_kv) + j] = half.T.astype(BF16)

    load_step(0, lambda i, vals: None)

    def q_steps(i, _):
        load_step(i, q_post)
        q_to_mirror(i - 1).start()
        q_to_sibling(i - 1).start()
        return 0
    lax.fori_loop(1, n_q + 1, q_steps, 0)

    def k_steps(i, _):
        load_step(i, k_post)
        return 0
    lax.fori_loop(n_q + 1, n_q + n_kv + 1, k_steps, 0)

    def v_steps(i, _):
        load_step(i, v_post)
        return 0
    lax.fori_loop(n_q + n_kv + 1, steps, v_steps, 0)
    v_post(steps - 1, cols[...])

    for h in range(heads):
        wide[0, pl.ds(h, rows, stride=heads), :] = k_new[h].astype(F32)
        wide[1, pl.ds(h, rows, stride=heads), :] = v_new[h].astype(F32).T
    k_out[...] = wide[0, 0:rows * heads, :].astype(BF16)
    v_out[...] = wide[1, 0:rows * heads, :].astype(BF16)

    for g in range(2):
        q_to_mirror(g).wait_recv()
        q_forward(g).start()
    q_to_sibling(0).wait_recv()
    q_forward(0).wait_recv()

    def sib_copy(kind, g):
        return remote(part.at[kind, g, 1], sib_recv.at[kind, g], sib_send.at[kind, g], sib_sem.at[kind, g], sibling)
    def mir_copy(g):
        return remote(comb.at[g], mir_recv.at[g], mir_send.at[g], mir_sem.at[g], mirror)

    def main_body():
        def q_cols(kind, g):
            base = 2 - 2 * kind
            return jnp.concatenate([qs[base, g], qs[base + 1, g]], axis=1)

        def dot(a, b):
            return lax.dot_general(a, b, (((1,), (0,)), ((), ())), preferred_element_type=F32)

        def col_max(mx, s):
            return jnp.maximum(mx, jnp.max(s.reshape(s.shape[0] // 8, 8, 512), axis=0))

        def qk(q, g, kc, slot, mx):
            s = dot(kh[g, pl.ds(pl.multiple_of(kc * KEY_TILE, KEY_TILE), KEY_TILE), :], q)
            SB[slot][kc] = s
            return col_max(mx, s)

        def qk_new(q, kind, g, slot, mx):
            own = lax.rem(me + 2 * (1 - kind), 4)
            other = lax.rem(sibling + 2 * (1 - kind), 4)
            key = lax.broadcasted_iota(jnp.int32, (rows, 512), 0) + me * rows
            col = lax.broadcasted_iota(jnp.int32, (rows, 512), 1)
            row = lax.rem(col, rows) + jnp.where(col < 256, own, other) * rows
            s = jnp.where(key <= row, dot(k_new[g], q), -jnp.inf)
            sN[slot] = s
            return col_max(mx, s)

        def weights(s, mc, ls):
            p = jnp.exp2(s * SCALE_LOG2 - mc)
            return p.astype(BF16), ls + jnp.sum(p.reshape(s.shape[0] // 8, 8, 512), axis=0)

        def block(last, kind_n, g_n, kind, g, b, par):
            steps = [("Q", i) for i in range(GROUP)] + [("Q", None)] * last
            for i in range(GROUP):
                steps.insert(LEAD + 2 * i, ("P", i))
            steps += [("P", None)] * last
            mx, ls, mc = mbuf[...], lbuf[...], mcb[par, 0:1, :]
            q = q_cols(kind_n, g_n)
            acc = None
            for op, i in steps:
                if op == "Q" and i is None:
                    mx = qk_new(q, kind_n, g_n, 1 - par, mx)
                elif op == "Q":
                    mx = qk(q, g_n, b * GROUP + i, 1 - par, mx)
                else:
                    if i is None:
                        p, ls = weights(sN[par], mc, ls)
                        v = v_new[g]
                    else:
                        kc = b * GROUP + i
                        p, ls = weights(SB[par][kc], mc, ls)
                        v = vt[g, :, pl.ds(pl.multiple_of(kc * KEY_TILE, KEY_TILE), KEY_TILE)]
                    pv = dot(v, p)
                    acc = pv if acc is None else acc + pv
            if not last:
                mbuf[...] = mx
                lbuf[...] = ls
                obuf[...] = acc
                return
            acc = obuf[...] + acc
            total = jnp.sum(ls, axis=0, keepdims=True)
            for t in range(2):
                part[kind, g, t, 0:128, :] = acc[:, TS(t)]
                part[kind, g, t, 128:129, :] = mc[:, TS(t)]
                part[kind, g, t, 129:130, :] = total[:, TS(t)]
            mcb[1 - par, 0:1, :] = jnp.max(mx, axis=0, keepdims=True) * SCALE_LOG2
            mbuf[...] = jnp.full(mbuf.shape, -jnp.inf, F32)
            lbuf[...] = jnp.zeros(lbuf.shape, F32)

        def merge(a, b):
            ma, mb = a[128:129, :], b[128:129, :]
            m = jnp.maximum(ma, mb)
            fa, fb = jnp.exp2(ma - m), jnp.exp2(mb - m)
            return a[0:128, :] * fa + b[0:128, :] * fb, m, a[129:130, :] * fa + b[129:130, :] * fb

        def send_merged(g):
            sib_copy(0, g).wait_recv()
            acc, m, total = merge(part.at[0, g, 0], sib_recv.at[0, g])
            comb[g, 0:128, :] = acc
            comb[g, 128:129, :] = m
            comb[g, 129:130, :] = total
            mir_copy(g).start()

        def unit_of(pos):
            half = pos // 2
            odd = pos - 2 * half
            local = jnp.where((odd == 0) & (half > 0) | (pos >= 2 * heads - 1), 1, 0)
            return local, jnp.where(pos >= 2 * heads - 1, heads - 1, jnp.maximum(half - 1 + 2 * odd, 0))

        def unit(p, par):
            pos = 2 * p + par
            kind, g = unit_of(pos)
            kind_n, g_n = unit_of(jnp.minimum(pos + 1, 2 * heads - 1))
            for b in range(tiles // GROUP):
                @pl.when(p < (2 + b) * heads)
                def _():
                    block(b == tiles // GROUP - 1, kind_n, g_n, kind, g, b, par)
                if b == 0:
                    @pl.when((p == 0) if par else (p > 0))
                    def _():
                        send_merged(p)
            sib_copy(kind, g).start()

        mbuf[...] = jnp.full(mbuf.shape, -jnp.inf, F32)
        q0 = q_cols(0, 0)
        def first(b, _):
            mx = mbuf[...]
            for c in range(4):
                mx = qk(q0, 0, 4 * b + c, 0, mx)
            mbuf[...] = mx
            return 0
        lax.fori_loop(0, tiles // 4, first, 0)
        mx = qk_new(q0, 0, 0, 0, mbuf[...])
        mcb[0, 0:1, :] = jnp.max(mx, axis=0, keepdims=True) * SCALE_LOG2
        mbuf[...] = jnp.full(mbuf.shape, -jnp.inf, F32)
        lbuf[...] = jnp.zeros(lbuf.shape, F32)

        def body(p, _):
            @pl.when(p + 1 < heads)
            def _():
                q_to_sibling(p + 1).wait_recv()
                q_forward(p + 1).wait_recv()
            unit(p, 0)
            @pl.when(p + 2 < heads)
            def _():
                q_to_mirror(p + 2).wait_recv()
                q_forward(p + 2).start()
            unit(p, 1)
            return 0
        lax.fori_loop(0, heads, body, 0)

        def final(g, _):
            sib_copy(1, g).wait_recv()
            mir_copy(g).wait_recv()
            acc, m, total = merge(part.at[1, g, 0], sib_recv.at[1, g])
            mb = mir_recv[g, 128:129, :]
            top = jnp.maximum(m, mb)
            fa, fb = jnp.exp2(m - top), jnp.exp2(mb - top)
            acc = acc * fa + mir_recv[g, 0:128, :] * fb
            total = total * fa + mir_recv[g, 129:130, :] * fb
            o = acc / total
            for j in range(2):
                cols = pl.ds(pl.multiple_of((2 * g + j) * 128, 128), 128)
                att[:, cols] = o[:, j * 128:(j + 1) * 128].T.astype(BF16)
            return 0
        lax.fori_loop(0, heads, final, 0)
        n_out = x_ref.shape[1] // 256
        def project(n, _):
            slot = lax.rem(n, WSLOTS)
            weight_copy(w_o, n, slot).wait()
            cols = pl.ds(pl.multiple_of(n * 256, 256), 256)
            add = jnp.dot(att[...], wbuf[slot], preferred_element_type=F32)
            out_ref[:, cols] = (x_ref[:, cols].astype(F32) + add).astype(BF16)
            @pl.when(n + WSLOTS < n_out)
            def _():
                weight_copy(w_o, n + WSLOTS, slot).start()
            return 0
        lax.fori_loop(0, n_out, project, 0)

    main_body()

    def drain(g, _):
        q_to_mirror(g).wait_send()
        q_to_sibling(g).wait_send()
        q_forward(g).wait_send()
        sib_copy(0, g).wait_send()
        sib_copy(1, g).wait_send()
        mir_copy(g).wait_send()
        return 0
    lax.fori_loop(0, heads, drain, 0)


def attention_block(x, ln_gain, q_gain, k_gain, cos_tab, sin_tab, w_q, w_k, w_v, w_o, k_cache, v_cache):
    n_keys, heads, _ = k_cache.shape
    rows, width = x.shape
    vm = pl.BlockSpec(memory_space=pltpu.VMEM)
    hbm = pl.BlockSpec(memory_space=pl.ANY)
    dma = pltpu.SemaphoreType.DMA
    tiles = n_keys // KEY_TILE
    return pl.pallas_call(
        functools.partial(block_kernel, n_keys, heads),
        out_shape=(jax.ShapeDtypeStruct((rows, width), BF16), jax.ShapeDtypeStruct((rows * heads, HEAD_DIM), BF16),
                   jax.ShapeDtypeStruct((rows * heads, HEAD_DIM), BF16)),
        in_specs=[vm] * 6 + [hbm] * 6,
        out_specs=(vm, vm, vm),
        scratch_shapes=[
            pltpu.VMEM((rows, width), BF16), pltpu.VMEM((WSLOTS, width, 256), BF16),
            pltpu.VMEM((rows, 256), F32), pltpu.VMEM((rows, 128), F32), pltpu.VMEM((rows, 128), F32), pltpu.VMEM((rows, w_o.shape[0]), BF16),
            pltpu.VMEM((heads, rows, 128), BF16), pltpu.VMEM((heads, 128, rows), BF16),
            pltpu.VMEM((heads, n_keys, 128), BF16), pltpu.VMEM((heads, 128, n_keys), BF16),
            pltpu.VMEM((tiles, KEY_TILE, 512), F32), pltpu.VMEM((tiles, KEY_TILE, 512), F32),
            pltpu.VMEM((2, rows, 512), F32),
            pltpu.VMEM((8, 512), F32), pltpu.VMEM((8, 512), F32), pltpu.VMEM((2, 8, 512), F32), pltpu.VMEM((128, 512), F32),
            pltpu.VMEM((4, heads, 128, 256), BF16),
            pltpu.VMEM((2, heads, 2, 136, 256), F32), pltpu.VMEM((2, heads, 136, 256), F32),
            pltpu.VMEM((heads, 136, 256), F32), pltpu.VMEM((heads, 136, 256), F32),
            pltpu.VMEM((2, CSLOTS, PREP * heads, 128), BF16), pltpu.VMEM((2, PREP * heads, 128), F32),
            dma((2, CSLOTS)), dma((WSLOTS,)), dma((3, heads)), dma((3, heads)), dma((2, heads)), dma((2, heads)), dma((heads,)), dma((heads,)),
        ],
        compiler_params=pltpu.CompilerParams(vmem_limit_bytes=62 * 2**20, collective_id=0, has_side_effects=True),
    )(x, ln_gain, q_gain, k_gain, cos_tab, sin_tab, w_q, w_k, w_v, w_o,
      k_cache.reshape(n_keys * heads, HEAD_DIM), v_cache.reshape(n_keys * heads, HEAD_DIM))


def pass_on(*arrays):
    def kernel(*refs):
        n = len(refs) // 2
        for src, dst in zip(refs[:n], refs[n:]):
            dst[...] = src[...]
    vm = pl.BlockSpec(memory_space=pltpu.VMEM)
    return pl.pallas_call(kernel, out_shape=tuple(jax.ShapeDtypeStruct(a.shape, a.dtype) for a in arrays),
                          in_specs=[vm] * len(arrays), out_specs=(vm,) * len(arrays))(*arrays)


def solution(mesh):
    cp_size = mesh.shape['cp']
    row_spec = P(('dp', 'cp'), None)
    cache_spec = P(('dp', 'cp'), None, None)
    whole = P()

    def device_step(x_rows, k_cache, v_cache, ln_gain, w_q, w_k, w_v, w_o, q_gain, k_gain):
        rows = x_rows.shape[0]
        n_keys, heads, _ = k_cache.shape
        positions = n_keys * cp_size + lax.axis_index('cp') * rows + jnp.arange(rows)
        cos_tab, sin_tab = rope_tables(positions)
        out, k_new, v_new = pass_on(*attention_block(x_rows, ln_gain, q_gain, k_gain, cos_tab, sin_tab, w_q, w_k, w_v, w_o, k_cache, v_cache))
        return out, k_new.reshape(rows, heads, HEAD_DIM), v_new.reshape(rows, heads, HEAD_DIM)

    return jax.shard_map(device_step, mesh=mesh, in_specs=(row_spec, cache_spec, cache_spec, whole, whole, whole, whole, whole, whole, whole), out_specs=(row_spec, cache_spec, cache_spec), check_vma=False)
```

```python
import functools
import math

import jax
import jax.numpy as jnp
from jax import lax
from jax.experimental import pallas as pl
from jax.experimental.pallas import tpu as pltpu
from jax.sharding import PartitionSpec as P

HEAD_DIM = 128
ROPE_THETA = 1.0e6
NORM_EPS = 1.0e-6
SCALE_LOG2 = HEAD_DIM ** -0.5 * math.log2(math.e)
F32, BF16 = jnp.float32, jnp.bfloat16
MESH = pl.DeviceIdType.MESH

KEY_TILE = 256
PREP = 256
GROUP = 16
HOIST = 64
WSLOTS = 4
CSLOTS = 4
LEAD = 1


def rope_tables(positions):
    half = HEAD_DIM // 2
    inv_freq = ROPE_THETA ** (-jnp.arange(half, dtype=F32) * (2.0 / HEAD_DIM))
    angles = positions.astype(F32)[:, None] * inv_freq[None, :]
    return jnp.cos(angles), jnp.sin(angles)


def block_kernel(n_keys, heads, x_ref, ln_gain, q_gain, k_gain, cos_tab, sin_tab, w_q, w_k, w_v, w_o, k_hbm, v_hbm,
                 out_ref, k_out, v_out,
                 hid, wbuf, cols, cosw, sinw, att, k_new, v_new,
                 kh, vt, sA, sB, sN, mbuf, lbuf, mcb, obuf, qs, part, sib_recv, comb, mir_recv, raw, wide,
                 copy_sem, w_sem, q_send, q_sem, sib_send, sib_sem, mir_send, mir_sem):
    SB = (sA, sB)
    me = lax.axis_index("cp")
    sibling = me + 1 - 2 * lax.rem(me, 2)
    mirror = lax.rem(me + 2, 4)
    rows = 128
    tiles = n_keys // KEY_TILE
    units = 2 * heads
    TS = lambda t: slice(t * 256, (t + 1) * 256)

    def remote(src, dst, send, recv, to):
        return pltpu.make_async_remote_copy(src_ref=src, dst_ref=dst, send_sem=send, recv_sem=recv,
                                            device_id={"cp": to}, device_id_type=MESH)

    def cache_copy(i, which, slot):
        src = (k_hbm, v_hbm)[which]
        n = PREP * heads
        return pltpu.make_async_copy(src.at[pl.ds(pl.multiple_of(i * n, n), n), :], raw.at[which, slot], copy_sem.at[which, slot])

    def weight_copy(w, c, slot):
        return pltpu.make_async_copy(w.at[:, pl.ds(pl.multiple_of(c * 256, 256), 256)], wbuf.at[slot], w_sem.at[slot])

    for c in range(WSLOTS):
        weight_copy(w_q, c, c).start()
    for s in range(CSLOTS):
        cache_copy(s, 0, s).start()
        cache_copy(s, 1, s).start()

    xw = x_ref[...].astype(F32)
    mean_sq = jnp.mean(xw * xw, axis=-1, keepdims=True)
    hid[...] = (xw * lax.rsqrt(mean_sq + NORM_EPS) * ln_gain[...].astype(F32).reshape(1, -1)).astype(BF16)
    cosw[...] = jnp.concatenate([cos_tab[...], cos_tab[...]], axis=1)
    sinw[...] = jnp.concatenate([-sin_tab[...], sin_tab[...]], axis=1)

    barrier = pltpu.get_barrier_semaphore()
    for peer in (sibling, mirror):
        pl.semaphore_signal(barrier, inc=1, device_id={"cp": peer}, device_id_type=MESH)
    pl.semaphore_wait(barrier, 2)

    def q_to_sibling(g):
        return remote(qs.at[0, g], qs.at[1, g], q_send.at[0, g], q_sem.at[0, g], sibling)
    def q_to_mirror(g):
        return remote(qs.at[0, g], qs.at[2, g], q_send.at[1, g], q_sem.at[1, g], mirror)
    def q_forward(g):
        return remote(qs.at[2, g], qs.at[3, g], q_send.at[2, g], q_sem.at[2, g], sibling)

    def prep(i):
        slot = lax.rem(i, CSLOTS)
        row = pl.ds(pl.multiple_of(i * PREP, PREP), PREP)
        wide[0] = raw[0, slot].astype(F32)
        for h in range(heads):
            kh[h, row, :] = wide[0, pl.ds(h, PREP, stride=heads), :].astype(BF16)
        wide[1] = raw[1, slot].astype(F32)
        for h in range(heads):
            vt[h, :, row] = wide[1, pl.ds(h, PREP, stride=heads), :].T.astype(BF16)

    def head_rows(vals, gain):
        vals = vals.astype(BF16).astype(F32)
        normed = vals * lax.rsqrt(jnp.mean(vals * vals, axis=-1, keepdims=True) + NORM_EPS) * gain
        return normed * cosw[...] + pltpu.roll(normed, HEAD_DIM // 2, 1) * sinw[...]

    n_q, n_kv = heads, heads // 2
    steps = n_q + 2 * n_kv

    def load_step(i, post):
        wslot = lax.rem(i, WSLOTS)
        slot = lax.rem(i, CSLOTS)
        weight_copy(w_q, 0, wslot).wait()
        cache_copy(i, 0, slot).wait()
        cache_copy(i, 1, slot).wait()
        done = cols[...]
        fresh = jnp.dot(hid[...], wbuf[wslot], preferred_element_type=F32)
        prep(i)
        post(i - 1, done)
        cols[...] = fresh
        ahead = i + WSLOTS
        for w, lo, hi in ((w_q, 0, n_q), (w_k, n_q, n_q + n_kv), (w_v, n_q + n_kv, steps), (w_o, steps, steps + WSLOTS)):
            @pl.when((ahead >= lo) & (ahead < hi))
            def _():
                weight_copy(w, ahead - lo, wslot).start()
        @pl.when(i + CSLOTS < n_keys // PREP)
        def _():
            cache_copy(i + CSLOTS, 0, slot).start()
            cache_copy(i + CSLOTS, 1, slot).start()

    def halves(vals):
        return [vals[:, j * 128:(j + 1) * 128] for j in range(2)]

    def q_post(g, vals):
        for j, half in enumerate(halves(vals)):
            qs[0, g, :, j * 128:(j + 1) * 128] = head_rows(half, q_gain[...].astype(F32).reshape(1, -1)).T.astype(BF16)

    def k_post(c, vals):
        for j, half in enumerate(halves(vals)):
            k_new[2 * (c - n_q) + j] = head_rows(half, k_gain[...].astype(F32).reshape(1, -1)).astype(BF16)

    def v_post(c, vals):
        for j, half in enumerate(halves(vals)):
            v_new[2 * (c - n_q - n_kv) + j] = half.T.astype(BF16)

    load_step(0, lambda i, vals: None)

    def q_steps(i, _):
        load_step(i, q_post)
        q_to_mirror(i - 1).start()
        q_to_sibling(i - 1).start()
        return 0
    lax.fori_loop(1, n_q + 1, q_steps, 0)

    def forward_q(g):
        q_to_mirror(g).wait_recv()
        q_forward(g).start()

    def k_steps(i, _):
        load_step(i, k_post)
        return 0
    lax.fori_loop(n_q + 1, n_q + n_kv + 1, k_steps, 0)

    def v_steps(i, _):
        load_step(i, v_post)
        forward_q(i - n_q - n_kv - 1)
        return 0
    lax.fori_loop(n_q + n_kv + 1, steps, v_steps, 0)
    v_post(steps - 1, cols[...])

    for h in range(heads):
        wide[0, pl.ds(h, rows, stride=heads), :] = k_new[h].astype(F32)
        wide[1, pl.ds(h, rows, stride=heads), :] = v_new[h].astype(F32).T
    k_out[...] = wide[0, 0:rows * heads, :].astype(BF16)
    v_out[...] = wide[1, 0:rows * heads, :].astype(BF16)

    def sibling_q(g, _):
        q_to_sibling(g).wait_recv()
        return 0
    lax.fori_loop(0, heads, sibling_q, 0)
    q_forward(0).wait_recv()
    q_forward(1).wait_recv()

    def sib_copy(kind, g):
        return remote(part.at[kind, g, 1], sib_recv.at[kind, g], sib_send.at[kind, g], sib_sem.at[kind, g], sibling)
    def mir_copy(g):
        return remote(comb.at[g], mir_recv.at[g], mir_send.at[g], mir_sem.at[g], mirror)

    def main_body():
        def q_cols(kind, g):
            base = 2 - 2 * kind
            return jnp.concatenate([qs[base, g], qs[base + 1, g]], axis=1)

        def dot(a, b):
            return lax.dot_general(a, b, (((1,), (0,)), ((), ())), preferred_element_type=F32)

        def col_max(mx, s):
            return jnp.maximum(mx, jnp.max(s.reshape(s.shape[0] // 8, 8, 512), axis=0))

        def qk(q, g, kc, slot, mx):
            s = dot(kh[g, pl.ds(pl.multiple_of(kc * KEY_TILE, KEY_TILE), KEY_TILE), :], q)
            SB[slot][kc] = s
            return col_max(mx, s)

        def qk_new(q, kind, g, slot, mx):
            own = lax.rem(me + 2 * (1 - kind), 4)
            other = lax.rem(sibling + 2 * (1 - kind), 4)
            key = lax.broadcasted_iota(jnp.int32, (rows, 512), 0) + me * rows
            col = lax.broadcasted_iota(jnp.int32, (rows, 512), 1)
            row = lax.rem(col, rows) + jnp.where(col < 256, own, other) * rows
            s = jnp.where(key <= row, dot(k_new[g], q), -jnp.inf)
            sN[slot] = s
            return col_max(mx, s)

        def weights(s, mc, ls):
            p = jnp.exp2(s * SCALE_LOG2 - mc)
            return p.astype(BF16), ls + jnp.sum(p.reshape(s.shape[0] // 8, 8, 512), axis=0)

        def block(last, kind_n, g_n, kind, g, b, par):
            steps = [("Q", i) for i in range(GROUP)] + [("Q", None)] * last
            for i in range(GROUP):
                steps.insert(LEAD + 2 * i, ("P", i))
            steps += [("P", None)] * last
            mx, ls, mc = mbuf[...], lbuf[...], mcb[par, 0:1, :]
            q = q_cols(kind_n, g_n)
            acc = None
            for op, i in steps:
                if op == "Q" and i is None:
                    mx = qk_new(q, kind_n, g_n, 1 - par, mx)
                elif op == "Q":
                    mx = qk(q, g_n, b * GROUP + i, 1 - par, mx)
                else:
                    if i is None:
                        p, ls = weights(sN[par], mc, ls)
                        v = v_new[g]
                    else:
                        kc = b * GROUP + i
                        p, ls = weights(SB[par][kc], mc, ls)
                        v = vt[g, :, pl.ds(pl.multiple_of(kc * KEY_TILE, KEY_TILE), KEY_TILE)]
                    pv = dot(v, p)
                    acc = pv if acc is None else acc + pv
            if not last:
                mbuf[...] = mx
                lbuf[...] = ls
                obuf[...] = acc
                return
            acc = obuf[...] + acc
            total = jnp.sum(ls, axis=0, keepdims=True)
            for t in range(2):
                part[kind, g, t, 0:128, :] = acc[:, TS(t)]
                part[kind, g, t, 128:129, :] = mc[:, TS(t)]
                part[kind, g, t, 129:130, :] = total[:, TS(t)]
            mcb[1 - par, 0:1, :] = jnp.max(mx, axis=0, keepdims=True) * SCALE_LOG2
            mbuf[...] = jnp.full(mbuf.shape, -jnp.inf, F32)
            lbuf[...] = jnp.zeros(lbuf.shape, F32)

        def merge(a, b):
            ma, mb = a[128:129, :], b[128:129, :]
            m = jnp.maximum(ma, mb)
            fa, fb = jnp.exp2(ma - m), jnp.exp2(mb - m)
            return a[0:128, :] * fa + b[0:128, :] * fb, m, a[129:130, :] * fa + b[129:130, :] * fb

        def send_merged(g):
            sib_copy(0, g).wait_recv()
            acc, m, total = merge(part.at[0, g, 0], sib_recv.at[0, g])
            comb[g, 0:128, :] = acc
            comb[g, 128:129, :] = m
            comb[g, 129:130, :] = total
            mir_copy(g).start()

        def unit_of(pos):
            half = pos // 2
            odd = pos - 2 * half
            local = jnp.where((odd == 1) & (half > 0) | (pos >= 2 * heads - 2), 1, 0)
            g = jnp.where(odd == 1, half - 1, half + 1)
            g = jnp.where(pos < 2, pos, jnp.where(pos >= 2 * heads - 2, pos - heads, g))
            return local, g

        def unit(p, par):
            pos = 2 * p + par
            kind, g = unit_of(pos)
            kind_n, g_n = unit_of(jnp.minimum(pos + 1, 2 * heads - 1))
            for b in range(tiles // GROUP):
                @pl.when(p < (2 + b) * heads)
                def _():
                    block(b == tiles // GROUP - 1, kind_n, g_n, kind, g, b, par)
                if b == 0:
                    @pl.when((p < heads - 1) if par else (p == 1))
                    def _():
                        send_merged(jnp.where(p == 0, 0, p + 1) if par else 1)
            sib_copy(kind, g).start()

        mbuf[...] = jnp.full(mbuf.shape, -jnp.inf, F32)
        q0 = q_cols(0, 0)
        def first(b, _):
            mx = mbuf[...]
            for c in range(4):
                mx = qk(q0, 0, 4 * b + c, 0, mx)
            mbuf[...] = mx
            return 0
        lax.fori_loop(0, tiles // 4, first, 0)
        mx = qk_new(q0, 0, 0, 0, mbuf[...])
        mcb[0, 0:1, :] = jnp.max(mx, axis=0, keepdims=True) * SCALE_LOG2
        mbuf[...] = jnp.full(mbuf.shape, -jnp.inf, F32)
        lbuf[...] = jnp.zeros(lbuf.shape, F32)

        def body(p, _):
            @pl.when(p + 3 < heads)
            def _():
                forward_q(p + 3)
            unit(p, 0)
            @pl.when(p + 2 < heads)
            def _():
                q_forward(p + 2).wait_recv()
            unit(p, 1)
            return 0
        lax.fori_loop(0, heads, body, 0)

        def final(g, _):
            sib_copy(1, g).wait_recv()
            mir_copy(g).wait_recv()
            acc, m, total = merge(part.at[1, g, 0], sib_recv.at[1, g])
            mb = mir_recv[g, 128:129, :]
            top = jnp.maximum(m, mb)
            fa, fb = jnp.exp2(m - top), jnp.exp2(mb - top)
            acc = acc * fa + mir_recv[g, 0:128, :] * fb
            total = total * fa + mir_recv[g, 129:130, :] * fb
            o = acc / total
            for j in range(2):
                cols = pl.ds(pl.multiple_of((2 * g + j) * 128, 128), 128)
                att[:, cols] = o[:, j * 128:(j + 1) * 128].T.astype(BF16)
            return 0
        lax.fori_loop(0, heads, final, 0)
        n_out = x_ref.shape[1] // 256
        def project(n, _):
            slot = lax.rem(n, WSLOTS)
            weight_copy(w_o, n, slot).wait()
            cols = pl.ds(pl.multiple_of(n * 256, 256), 256)
            add = jnp.dot(att[...], wbuf[slot], preferred_element_type=F32)
            out_ref[:, cols] = (x_ref[:, cols].astype(F32) + add).astype(BF16)
            @pl.when(n + WSLOTS < n_out)
            def _():
                weight_copy(w_o, n + WSLOTS, slot).start()
            return 0
        lax.fori_loop(0, n_out, project, 0)

    main_body()

    def drain(g, _):
        q_to_mirror(g).wait_send()
        q_to_sibling(g).wait_send()
        q_forward(g).wait_send()
        sib_copy(0, g).wait_send()
        sib_copy(1, g).wait_send()
        mir_copy(g).wait_send()
        return 0
    lax.fori_loop(0, heads, drain, 0)


def attention_block(x, ln_gain, q_gain, k_gain, cos_tab, sin_tab, w_q, w_k, w_v, w_o, k_cache, v_cache):
    n_keys, heads, _ = k_cache.shape
    rows, width = x.shape
    vm = pl.BlockSpec(memory_space=pltpu.VMEM)
    hbm = pl.BlockSpec(memory_space=pl.ANY)
    dma = pltpu.SemaphoreType.DMA
    tiles = n_keys // KEY_TILE
    return pl.pallas_call(
        functools.partial(block_kernel, n_keys, heads),
        out_shape=(jax.ShapeDtypeStruct((rows, width), BF16), jax.ShapeDtypeStruct((rows * heads, HEAD_DIM), BF16),
                   jax.ShapeDtypeStruct((rows * heads, HEAD_DIM), BF16)),
        in_specs=[vm] * 6 + [hbm] * 6,
        out_specs=(vm, vm, vm),
        scratch_shapes=[
            pltpu.VMEM((rows, width), BF16), pltpu.VMEM((WSLOTS, width, 256), BF16),
            pltpu.VMEM((rows, 256), F32), pltpu.VMEM((rows, 128), F32), pltpu.VMEM((rows, 128), F32), pltpu.VMEM((rows, w_o.shape[0]), BF16),
            pltpu.VMEM((heads, rows, 128), BF16), pltpu.VMEM((heads, 128, rows), BF16),
            pltpu.VMEM((heads, n_keys, 128), BF16), pltpu.VMEM((heads, 128, n_keys), BF16),
            pltpu.VMEM((tiles, KEY_TILE, 512), F32), pltpu.VMEM((tiles, KEY_TILE, 512), F32),
            pltpu.VMEM((2, rows, 512), F32),
            pltpu.VMEM((8, 512), F32), pltpu.VMEM((8, 512), F32), pltpu.VMEM((2, 8, 512), F32), pltpu.VMEM((128, 512), F32),
            pltpu.VMEM((4, heads, 128, 256), BF16),
            pltpu.VMEM((2, heads, 2, 136, 256), F32), pltpu.VMEM((2, heads, 136, 256), F32),
            pltpu.VMEM((heads, 136, 256), F32), pltpu.VMEM((heads, 136, 256), F32),
            pltpu.VMEM((2, CSLOTS, PREP * heads, 128), BF16), pltpu.VMEM((2, PREP * heads, 128), F32),
            dma((2, CSLOTS)), dma((WSLOTS,)), dma((3, heads)), dma((3, heads)), dma((2, heads)), dma((2, heads)), dma((heads,)), dma((heads,)),
        ],
        compiler_params=pltpu.CompilerParams(vmem_limit_bytes=62 * 2**20, collective_id=0, has_side_effects=True),
    )(x, ln_gain, q_gain, k_gain, cos_tab, sin_tab, w_q, w_k, w_v, w_o,
      k_cache.reshape(n_keys * heads, HEAD_DIM), v_cache.reshape(n_keys * heads, HEAD_DIM))


def pass_on(*arrays):
    def kernel(*refs):
        n = len(refs) // 2
        for src, dst in zip(refs[:n], refs[n:]):
            dst[...] = src[...]
    vm = pl.BlockSpec(memory_space=pltpu.VMEM)
    return pl.pallas_call(kernel, out_shape=tuple(jax.ShapeDtypeStruct(a.shape, a.dtype) for a in arrays),
                          in_specs=[vm] * len(arrays), out_specs=(vm,) * len(arrays))(*arrays)


def solution(mesh):
    cp_size = mesh.shape['cp']
    row_spec = P(('dp', 'cp'), None)
    cache_spec = P(('dp', 'cp'), None, None)
    whole = P()

    def device_step(x_rows, k_cache, v_cache, ln_gain, w_q, w_k, w_v, w_o, q_gain, k_gain):
        rows = x_rows.shape[0]
        n_keys, heads, _ = k_cache.shape
        positions = n_keys * cp_size + lax.axis_index('cp') * rows + jnp.arange(rows)
        cos_tab, sin_tab = rope_tables(positions)
        out, k_new, v_new = pass_on(*attention_block(x_rows, ln_gain, q_gain, k_gain, cos_tab, sin_tab, w_q, w_k, w_v, w_o, k_cache, v_cache))
        return out, k_new.reshape(rows, heads, HEAD_DIM), v_new.reshape(rows, heads, HEAD_DIM)

    return jax.shard_map(device_step, mesh=mesh, in_specs=(row_spec, cache_spec, cache_spec, whole, whole, whole, whole, whole, whole, whole), out_specs=(row_spec, cache_spec, cache_spec), check_vma=False)
```

```python
import functools
import math

import jax
import jax.numpy as jnp
from jax import lax
from jax.experimental import pallas as pl
from jax.experimental.pallas import tpu as pltpu
from jax.sharding import PartitionSpec as P

HEAD_DIM = 128
ROPE_THETA = 1.0e6
NORM_EPS = 1.0e-6
SCALE_LOG2 = HEAD_DIM ** -0.5 * math.log2(math.e)
F32, BF16 = jnp.float32, jnp.bfloat16
MESH = pl.DeviceIdType.MESH

KEY_TILE = 256
PREP = 256
GROUP = 16
HOIST = 64
WSLOTS = 4
CSLOTS = 4
LEAD = 1


def rope_tables(positions):
    half = HEAD_DIM // 2
    inv_freq = ROPE_THETA ** (-jnp.arange(half, dtype=F32) * (2.0 / HEAD_DIM))
    angles = positions.astype(F32)[:, None] * inv_freq[None, :]
    return jnp.cos(angles), jnp.sin(angles)


def block_kernel(n_keys, heads, x_ref, ln_gain, q_gain, k_gain, cos_tab, sin_tab, w_q, w_k, w_v, w_o, k_hbm, v_hbm,
                 out_ref, k_out, v_out,
                 hid, wbuf, cols, cosw, sinw, att, k_new, v_new,
                 kh, vt, sA, sB, sN, mbuf, lbuf, mcb, obuf, qs, part, sib_recv, comb, mir_recv, raw, wide,
                 copy_sem, w_sem, q_send, q_sem, sib_send, sib_sem, mir_send, mir_sem):
    SB = (sA, sB)
    me = lax.axis_index("cp")
    sibling = me + 1 - 2 * lax.rem(me, 2)
    mirror = lax.rem(me + 2, 4)
    rows = 128
    tiles = n_keys // KEY_TILE
    units = 2 * heads
    TS = lambda t: slice(t * 256, (t + 1) * 256)

    def remote(src, dst, send, recv, to):
        return pltpu.make_async_remote_copy(src_ref=src, dst_ref=dst, send_sem=send, recv_sem=recv,
                                            device_id={"cp": to}, device_id_type=MESH)

    def cache_copy(i, which, slot):
        src = (k_hbm, v_hbm)[which]
        n = PREP * heads
        return pltpu.make_async_copy(src.at[pl.ds(pl.multiple_of(i * n, n), n), :], raw.at[which, slot], copy_sem.at[which, slot])

    def weight_copy(w, c, slot):
        return pltpu.make_async_copy(w.at[:, pl.ds(pl.multiple_of(c * 256, 256), 256)], wbuf.at[slot], w_sem.at[slot])

    for c in range(WSLOTS):
        weight_copy(w_q, c, c).start()
    for s in range(CSLOTS):
        cache_copy(s, 0, s).start()
        cache_copy(s, 1, s).start()

    xw = x_ref[...].astype(F32)
    mean_sq = jnp.mean(xw * xw, axis=-1, keepdims=True)
    hid[...] = (xw * lax.rsqrt(mean_sq + NORM_EPS) * ln_gain[...].astype(F32).reshape(1, -1)).astype(BF16)
    cosw[...] = jnp.concatenate([cos_tab[...], cos_tab[...]], axis=1)
    sinw[...] = jnp.concatenate([-sin_tab[...], sin_tab[...]], axis=1)

    barrier = pltpu.get_barrier_semaphore()
    for peer in (sibling, mirror):
        pl.semaphore_signal(barrier, inc=1, device_id={"cp": peer}, device_id_type=MESH)
    pl.semaphore_wait(barrier, 2)

    def q_to_sibling(g):
        return remote(qs.at[0, g], qs.at[1, g], q_send.at[0, g], q_sem.at[0, g], sibling)
    def q_to_mirror(g):
        return remote(qs.at[0, g], qs.at[2, g], q_send.at[1, g], q_sem.at[1, g], mirror)
    def q_forward(g):
        return remote(qs.at[2, g], qs.at[3, g], q_send.at[2, g], q_sem.at[2, g], sibling)

    def prep(i):
        slot = lax.rem(i, CSLOTS)
        row = pl.ds(pl.multiple_of(i * PREP, PREP), PREP)
        wide[0] = raw[0, slot].astype(F32)
        for h in range(heads):
            kh[h, row, :] = wide[0, pl.ds(h, PREP, stride=heads), :].astype(BF16)
        wide[1] = raw[1, slot].astype(F32)
        for h in range(heads):
            vt[h, :, row] = wide[1, pl.ds(h, PREP, stride=heads), :].T.astype(BF16)

    def head_rows(vals, gain):
        vals = vals.astype(BF16).astype(F32)
        normed = vals * lax.rsqrt(jnp.mean(vals * vals, axis=-1, keepdims=True) + NORM_EPS) * gain
        return normed * cosw[...] + pltpu.roll(normed, HEAD_DIM // 2, 1) * sinw[...]

    n_q, n_kv = heads, heads // 2
    steps = n_q + 2 * n_kv

    def load_step(i, post):
        wslot = lax.rem(i, WSLOTS)
        slot = lax.rem(i, CSLOTS)
        weight_copy(w_q, 0, wslot).wait()
        cache_copy(i, 0, slot).wait()
        cache_copy(i, 1, slot).wait()
        done = cols[...]
        fresh = jnp.dot(hid[...], wbuf[wslot], preferred_element_type=F32)
        prep(i)
        post(i - 1, done)
        cols[...] = fresh
        ahead = i + WSLOTS
        for w, lo, hi in ((w_q, 0, n_q), (w_k, n_q, n_q + n_kv), (w_v, n_q + n_kv, steps), (w_o, steps, steps + WSLOTS)):
            @pl.when((ahead >= lo) & (ahead < hi))
            def _():
                weight_copy(w, ahead - lo, wslot).start()
        @pl.when(i + CSLOTS < n_keys // PREP)
        def _():
            cache_copy(i + CSLOTS, 0, slot).start()
            cache_copy(i + CSLOTS, 1, slot).start()

    def halves(vals):
        return [vals[:, j * 128:(j + 1) * 128] for j in range(2)]

    def q_post(g, vals):
        for j, half in enumerate(halves(vals)):
            qs[0, g, :, j * 128:(j + 1) * 128] = head_rows(half, q_gain[...].astype(F32).reshape(1, -1)).T.astype(BF16)

    def k_post(c, vals):
        for j, half in enumerate(halves(vals)):
            k_new[2 * (c - n_q) + j] = head_rows(half, k_gain[...].astype(F32).reshape(1, -1)).astype(BF16)

    def v_post(c, vals):
        for j, half in enumerate(halves(vals)):
            v_new[2 * (c - n_q - n_kv) + j] = half.T.astype(BF16)

    load_step(0, lambda i, vals: None)

    def q_steps(i, _):
        load_step(i, q_post)
        q_to_mirror(i - 1).start()
        q_to_sibling(i - 1).start()
        return 0
    lax.fori_loop(1, n_q + 1, q_steps, 0)

    def forward_q(g):
        q_to_mirror(g).wait_recv()
        q_forward(g).start()

    def k_steps(i, _):
        load_step(i, k_post)
        return 0
    lax.fori_loop(n_q + 1, n_q + n_kv + 1, k_steps, 0)

    def v_steps(i, _):
        load_step(i, v_post)
        forward_q(i - n_q - n_kv - 1)
        return 0
    lax.fori_loop(n_q + n_kv + 1, steps, v_steps, 0)
    v_post(steps - 1, cols[...])

    for h in range(heads):
        wide[0, pl.ds(h, rows, stride=heads), :] = k_new[h].astype(F32)
        wide[1, pl.ds(h, rows, stride=heads), :] = v_new[h].astype(F32).T
    k_out[...] = wide[0, 0:rows * heads, :].astype(BF16)
    v_out[...] = wide[1, 0:rows * heads, :].astype(BF16)

    def sibling_q(g, _):
        q_to_sibling(g).wait_recv()
        return 0
    lax.fori_loop(0, heads, sibling_q, 0)
    q_forward(0).wait_recv()
    q_forward(1).wait_recv()

    def sib_copy(kind, g):
        return remote(part.at[kind, g, 1], sib_recv.at[kind, g], sib_send.at[kind, g], sib_sem.at[kind, g], sibling)
    def mir_copy(g):
        return remote(comb.at[g], mir_recv.at[g], mir_send.at[g], mir_sem.at[g], mirror)

    def main_body():
        def q_cols(kind, g):
            base = 2 - 2 * kind
            return jnp.concatenate([qs[base, g], qs[base + 1, g]], axis=1)

        def dot(a, b):
            return lax.dot_general(a, b, (((1,), (0,)), ((), ())), preferred_element_type=F32)

        def col_max(mx, s):
            return jnp.maximum(mx, jnp.max(s.reshape(s.shape[0] // 8, 8, 512), axis=0))

        def qk(q, g, kc, slot, mx):
            s = dot(kh[g, pl.ds(pl.multiple_of(kc * KEY_TILE, KEY_TILE), KEY_TILE), :], q)
            SB[slot][kc] = s
            return col_max(mx, s)

        def qk_new(q, kind, g, slot, mx):
            own = lax.rem(me + 2 * (1 - kind), 4)
            other = lax.rem(sibling + 2 * (1 - kind), 4)
            key = lax.broadcasted_iota(jnp.int32, (rows, 512), 0) + me * rows
            col = lax.broadcasted_iota(jnp.int32, (rows, 512), 1)
            row = lax.rem(col, rows) + jnp.where(col < 256, own, other) * rows
            s = jnp.where(key <= row, dot(k_new[g], q), -jnp.inf)
            sN[slot] = s
            return col_max(mx, s)

        def weights(s, mc, ls):
            p = jnp.exp2(s * SCALE_LOG2 - mc)
            return p.astype(BF16), ls + jnp.sum(p.reshape(s.shape[0] // 8, 8, 512), axis=0)

        def block(last, kind_n, g_n, kind, g, b, par):
            steps = [("Q", i) for i in range(GROUP)] + [("Q", None)] * last
            for i in range(GROUP):
                steps.insert(LEAD + 2 * i, ("P", i))
            steps += [("P", None)] * last
            mx, ls, mc = mbuf[...], lbuf[...], mcb[par, 0:1, :]
            q = q_cols(kind_n, g_n)
            acc = None
            for op, i in steps:
                if op == "Q" and i is None:
                    mx = qk_new(q, kind_n, g_n, 1 - par, mx)
                elif op == "Q":
                    mx = qk(q, g_n, b * GROUP + i, 1 - par, mx)
                else:
                    if i is None:
                        p, ls = weights(sN[par], mc, ls)
                        v = v_new[g]
                    else:
                        kc = b * GROUP + i
                        p, ls = weights(SB[par][kc], mc, ls)
                        v = vt[g, :, pl.ds(pl.multiple_of(kc * KEY_TILE, KEY_TILE), KEY_TILE)]
                    pv = dot(v, p)
                    acc = pv if acc is None else acc + pv
            if not last:
                mbuf[...] = mx
                lbuf[...] = ls
                obuf[...] = acc
                return
            acc = obuf[...] + acc
            total = jnp.sum(ls, axis=0, keepdims=True)
            for t in range(2):
                part[kind, g, t, 0:128, :] = acc[:, TS(t)]
                part[kind, g, t, 128:129, :] = mc[:, TS(t)]
                part[kind, g, t, 129:130, :] = total[:, TS(t)]
            mcb[1 - par, 0:1, :] = jnp.max(mx, axis=0, keepdims=True) * SCALE_LOG2
            mbuf[...] = jnp.full(mbuf.shape, -jnp.inf, F32)
            lbuf[...] = jnp.zeros(lbuf.shape, F32)

        def merge(a, b):
            ma, mb = a[128:129, :], b[128:129, :]
            m = jnp.maximum(ma, mb)
            fa, fb = jnp.exp2(ma - m), jnp.exp2(mb - m)
            return a[0:128, :] * fa + b[0:128, :] * fb, m, a[129:130, :] * fa + b[129:130, :] * fb

        def send_merged(g):
            sib_copy(0, g).wait_recv()
            acc, m, total = merge(part.at[0, g, 0], sib_recv.at[0, g])
            comb[g, 0:128, :] = acc
            comb[g, 128:129, :] = m
            comb[g, 129:130, :] = total
            mir_copy(g).start()

        def unit_of(pos):
            half = pos // 2
            odd = pos - 2 * half
            local = jnp.where((odd == 1) & (half > 0) | (pos >= 2 * heads - 2), 1, 0)
            g = jnp.where(odd == 1, half - 1, half + 1)
            g = jnp.where(pos < 2, pos, jnp.where(pos >= 2 * heads - 2, pos - heads, g))
            return local, g

        def unit(p, par):
            pos = 2 * p + par
            kind, g = unit_of(pos)
            kind_n, g_n = unit_of(jnp.minimum(pos + 1, 2 * heads - 1))
            for b in range(tiles // GROUP):
                @pl.when(p < (2 + b) * heads)
                def _():
                    block(b == tiles // GROUP - 1, kind_n, g_n, kind, g, b, par)
                if b == 0:
                    @pl.when((p < heads - 1) if par else (p == 1))
                    def _():
                        send_merged(jnp.where(p == 0, 0, p + 1) if par else 1)
            sib_copy(kind, g).start()

        mbuf[...] = jnp.full(mbuf.shape, -jnp.inf, F32)
        q0 = q_cols(0, 0)
        def first(b, _):
            mx = mbuf[...]
            for c in range(16):
                mx = qk(q0, 0, 16 * b + c, 0, mx)
            mbuf[...] = mx
            return 0
        lax.fori_loop(0, tiles // 16, first, 0)
        mx = qk_new(q0, 0, 0, 0, mbuf[...])
        mcb[0, 0:1, :] = jnp.max(mx, axis=0, keepdims=True) * SCALE_LOG2
        mbuf[...] = jnp.full(mbuf.shape, -jnp.inf, F32)
        lbuf[...] = jnp.zeros(lbuf.shape, F32)

        def body(p, _):
            @pl.when(p + 3 < heads)
            def _():
                forward_q(p + 3)
            unit(p, 0)
            @pl.when(p + 2 < heads)
            def _():
                q_forward(p + 2).wait_recv()
            unit(p, 1)
            return 0
        lax.fori_loop(0, heads, body, 0)

        def final(g, _):
            sib_copy(1, g).wait_recv()
            mir_copy(g).wait_recv()
            acc, m, total = merge(part.at[1, g, 0], sib_recv.at[1, g])
            mb = mir_recv[g, 128:129, :]
            top = jnp.maximum(m, mb)
            fa, fb = jnp.exp2(m - top), jnp.exp2(mb - top)
            acc = acc * fa + mir_recv[g, 0:128, :] * fb
            total = total * fa + mir_recv[g, 129:130, :] * fb
            o = acc / total
            for j in range(2):
                cols = pl.ds(pl.multiple_of((2 * g + j) * 128, 128), 128)
                att[:, cols] = o[:, j * 128:(j + 1) * 128].T.astype(BF16)
            return 0
        lax.fori_loop(0, heads, final, 0)
        n_out = x_ref.shape[1] // 256
        def project(n, _):
            slot = lax.rem(n, WSLOTS)
            weight_copy(w_o, n, slot).wait()
            cols = pl.ds(pl.multiple_of(n * 256, 256), 256)
            add = jnp.dot(att[...], wbuf[slot], preferred_element_type=F32)
            out_ref[:, cols] = (x_ref[:, cols].astype(F32) + add).astype(BF16)
            @pl.when(n + WSLOTS < n_out)
            def _():
                weight_copy(w_o, n + WSLOTS, slot).start()
            return 0
        lax.fori_loop(0, n_out, project, 0)

    main_body()

    def drain(g, _):
        q_to_mirror(g).wait_send()
        q_to_sibling(g).wait_send()
        q_forward(g).wait_send()
        sib_copy(0, g).wait_send()
        sib_copy(1, g).wait_send()
        mir_copy(g).wait_send()
        return 0
    lax.fori_loop(0, heads, drain, 0)


def attention_block(x, ln_gain, q_gain, k_gain, cos_tab, sin_tab, w_q, w_k, w_v, w_o, k_cache, v_cache):
    n_keys, heads, _ = k_cache.shape
    rows, width = x.shape
    vm = pl.BlockSpec(memory_space=pltpu.VMEM)
    hbm = pl.BlockSpec(memory_space=pl.ANY)
    dma = pltpu.SemaphoreType.DMA
    tiles = n_keys // KEY_TILE
    return pl.pallas_call(
        functools.partial(block_kernel, n_keys, heads),
        out_shape=(jax.ShapeDtypeStruct((rows, width), BF16), jax.ShapeDtypeStruct((rows * heads, HEAD_DIM), BF16),
                   jax.ShapeDtypeStruct((rows * heads, HEAD_DIM), BF16)),
        in_specs=[vm] * 6 + [hbm] * 6,
        out_specs=(vm, vm, vm),
        scratch_shapes=[
            pltpu.VMEM((rows, width), BF16), pltpu.VMEM((WSLOTS, width, 256), BF16),
            pltpu.VMEM((rows, 256), F32), pltpu.VMEM((rows, 128), F32), pltpu.VMEM((rows, 128), F32), pltpu.VMEM((rows, w_o.shape[0]), BF16),
            pltpu.VMEM((heads, rows, 128), BF16), pltpu.VMEM((heads, 128, rows), BF16),
            pltpu.VMEM((heads, n_keys, 128), BF16), pltpu.VMEM((heads, 128, n_keys), BF16),
            pltpu.VMEM((tiles, KEY_TILE, 512), F32), pltpu.VMEM((tiles, KEY_TILE, 512), F32),
            pltpu.VMEM((2, rows, 512), F32),
            pltpu.VMEM((8, 512), F32), pltpu.VMEM((8, 512), F32), pltpu.VMEM((2, 8, 512), F32), pltpu.VMEM((128, 512), F32),
            pltpu.VMEM((4, heads, 128, 256), BF16),
            pltpu.VMEM((2, heads, 2, 136, 256), F32), pltpu.VMEM((2, heads, 136, 256), F32),
            pltpu.VMEM((heads, 136, 256), F32), pltpu.VMEM((heads, 136, 256), F32),
            pltpu.VMEM((2, CSLOTS, PREP * heads, 128), BF16), pltpu.VMEM((2, PREP * heads, 128), F32),
            dma((2, CSLOTS)), dma((WSLOTS,)), dma((3, heads)), dma((3, heads)), dma((2, heads)), dma((2, heads)), dma((heads,)), dma((heads,)),
        ],
        compiler_params=pltpu.CompilerParams(vmem_limit_bytes=62 * 2**20, collective_id=0, has_side_effects=True),
    )(x, ln_gain, q_gain, k_gain, cos_tab, sin_tab, w_q, w_k, w_v, w_o,
      k_cache.reshape(n_keys * heads, HEAD_DIM), v_cache.reshape(n_keys * heads, HEAD_DIM))


def pass_on(*arrays):
    def kernel(*refs):
        n = len(refs) // 2
        for src, dst in zip(refs[:n], refs[n:]):
            dst[...] = src[...]
    vm = pl.BlockSpec(memory_space=pltpu.VMEM)
    return pl.pallas_call(kernel, out_shape=tuple(jax.ShapeDtypeStruct(a.shape, a.dtype) for a in arrays),
                          in_specs=[vm] * len(arrays), out_specs=(vm,) * len(arrays))(*arrays)


def solution(mesh):
    cp_size = mesh.shape['cp']
    row_spec = P(('dp', 'cp'), None)
    cache_spec = P(('dp', 'cp'), None, None)
    whole = P()

    def device_step(x_rows, k_cache, v_cache, ln_gain, w_q, w_k, w_v, w_o, q_gain, k_gain):
        rows = x_rows.shape[0]
        n_keys, heads, _ = k_cache.shape
        positions = n_keys * cp_size + lax.axis_index('cp') * rows + jnp.arange(rows)
        cos_tab, sin_tab = rope_tables(positions)
        out, k_new, v_new = pass_on(*attention_block(x_rows, ln_gain, q_gain, k_gain, cos_tab, sin_tab, w_q, w_k, w_v, w_o, k_cache, v_cache))
        return out, k_new.reshape(rows, heads, HEAD_DIM), v_new.reshape(rows, heads, HEAD_DIM)

    return jax.shard_map(device_step, mesh=mesh, in_specs=(row_spec, cache_spec, cache_spec, whole, whole, whole, whole, whole, whole, whole), out_specs=(row_spec, cache_spec, cache_spec), check_vma=False)
```

```python
import functools
import math

import jax
import jax.numpy as jnp
from jax import lax
from jax.experimental import pallas as pl
from jax.experimental.pallas import tpu as pltpu
from jax.sharding import PartitionSpec as P

HEAD_DIM = 128
ROPE_THETA = 1.0e6
NORM_EPS = 1.0e-6
SCALE_LOG2 = HEAD_DIM ** -0.5 * math.log2(math.e)
F32, BF16 = jnp.float32, jnp.bfloat16
MESH = pl.DeviceIdType.MESH

KEY_TILE = 256
PREP = 256
GROUP = 16
HOIST = 64
WSLOTS = 6
CSLOTS = 4
LEAD = 1


def rope_tables(positions):
    half = HEAD_DIM // 2
    inv_freq = ROPE_THETA ** (-jnp.arange(half, dtype=F32) * (2.0 / HEAD_DIM))
    angles = positions.astype(F32)[:, None] * inv_freq[None, :]
    return jnp.cos(angles), jnp.sin(angles)


def block_kernel(n_keys, heads, x_ref, ln_gain, q_gain, k_gain, cos_tab, sin_tab, w_q, w_k, w_v, w_o, k_hbm, v_hbm,
                 out_ref, k_out, v_out,
                 hid, wbuf, cols, cosw, sinw, att, k_new, v_new,
                 kh, vt, sA, sB, sN, mbuf, lbuf, mcb, obuf, qs, part, sib_recv, comb, mir_recv, raw, wide,
                 copy_sem, w_sem, q_send, q_sem, sib_send, sib_sem, mir_send, mir_sem):
    SB = (sA, sB)
    me = lax.axis_index("cp")
    sibling = me + 1 - 2 * lax.rem(me, 2)
    mirror = lax.rem(me + 2, 4)
    rows = 128
    tiles = n_keys // KEY_TILE
    units = 2 * heads
    TS = lambda t: slice(t * 256, (t + 1) * 256)

    def remote(src, dst, send, recv, to):
        return pltpu.make_async_remote_copy(src_ref=src, dst_ref=dst, send_sem=send, recv_sem=recv,
                                            device_id={"cp": to}, device_id_type=MESH)

    def cache_copy(i, which, slot):
        src = (k_hbm, v_hbm)[which]
        n = PREP * heads
        return pltpu.make_async_copy(src.at[pl.ds(pl.multiple_of(i * n, n), n), :], raw.at[which, slot], copy_sem.at[which, slot])

    def weight_copy(w, c, slot):
        return pltpu.make_async_copy(w.at[:, pl.ds(pl.multiple_of(c * 256, 256), 256)], wbuf.at[slot], w_sem.at[slot])

    for c in range(WSLOTS):
        weight_copy(w_q, c, c).start()
    for s in range(CSLOTS):
        cache_copy(s, 0, s).start()
        cache_copy(s, 1, s).start()

    xw = x_ref[...].astype(F32)
    mean_sq = jnp.mean(xw * xw, axis=-1, keepdims=True)
    hid[...] = (xw * lax.rsqrt(mean_sq + NORM_EPS) * ln_gain[...].astype(F32).reshape(1, -1)).astype(BF16)
    cosw[...] = jnp.concatenate([cos_tab[...], cos_tab[...]], axis=1)
    sinw[...] = jnp.concatenate([-sin_tab[...], sin_tab[...]], axis=1)

    barrier = pltpu.get_barrier_semaphore()
    for peer in (sibling, mirror):
        pl.semaphore_signal(barrier, inc=1, device_id={"cp": peer}, device_id_type=MESH)
    pl.semaphore_wait(barrier, 2)

    def q_to_sibling(g):
        return remote(qs.at[0, g], qs.at[1, g], q_send.at[0, g], q_sem.at[0, g], sibling)
    def q_to_mirror(g):
        return remote(qs.at[0, g], qs.at[2, g], q_send.at[1, g], q_sem.at[1, g], mirror)
    def q_forward(g):
        return remote(qs.at[2, g], qs.at[3, g], q_send.at[2, g], q_sem.at[2, g], sibling)

    def prep(i):
        slot = lax.rem(i, CSLOTS)
        row = pl.ds(pl.multiple_of(i * PREP, PREP), PREP)
        wide[0] = raw[0, slot].astype(F32)
        for h in range(heads):
            kh[h, row, :] = wide[0, pl.ds(h, PREP, stride=heads), :].astype(BF16)
        wide[1] = raw[1, slot].astype(F32)
        for h in range(heads):
            vt[h, :, row] = wide[1, pl.ds(h, PREP, stride=heads), :].T.astype(BF16)

    def head_rows(vals, gain):
        vals = vals.astype(BF16).astype(F32)
        normed = vals * lax.rsqrt(jnp.mean(vals * vals, axis=-1, keepdims=True) + NORM_EPS) * gain
        return normed * cosw[...] + pltpu.roll(normed, HEAD_DIM // 2, 1) * sinw[...]

    n_q, n_kv = heads, heads // 2
    steps = n_q + 2 * n_kv

    def load_step(i, post):
        wslot = lax.rem(i, WSLOTS)
        slot = lax.rem(i, CSLOTS)
        weight_copy(w_q, 0, wslot).wait()
        cache_copy(i, 0, slot).wait()
        cache_copy(i, 1, slot).wait()
        done = cols[...]
        fresh = jnp.dot(hid[...], wbuf[wslot], preferred_element_type=F32)
        prep(i)
        post(i - 1, done)
        cols[...] = fresh
        ahead = i + WSLOTS
        for w, lo, hi in ((w_q, 0, n_q), (w_k, n_q, n_q + n_kv), (w_v, n_q + n_kv, steps), (w_o, steps, steps + WSLOTS)):
            @pl.when((ahead >= lo) & (ahead < hi))
            def _():
                weight_copy(w, ahead - lo, wslot).start()
        @pl.when(i + CSLOTS < n_keys // PREP)
        def _():
            cache_copy(i + CSLOTS, 0, slot).start()
            cache_copy(i + CSLOTS, 1, slot).start()

    def halves(vals):
        return [vals[:, j * 128:(j + 1) * 128] for j in range(2)]

    def q_post(g, vals):
        for j, half in enumerate(halves(vals)):
            qs[0, g, :, j * 128:(j + 1) * 128] = head_rows(half, q_gain[...].astype(F32).reshape(1, -1)).T.astype(BF16)

    def k_post(c, vals):
        for j, half in enumerate(halves(vals)):
            k_new[2 * (c - n_q) + j] = head_rows(half, k_gain[...].astype(F32).reshape(1, -1)).astype(BF16)

    def v_post(c, vals):
        for j, half in enumerate(halves(vals)):
            v_new[2 * (c - n_q - n_kv) + j] = half.T.astype(BF16)

    load_step(0, lambda i, vals: None)

    def q_steps(i, _):
        load_step(i, q_post)
        q_to_mirror(i - 1).start()
        q_to_sibling(i - 1).start()
        return 0
    lax.fori_loop(1, n_q + 1, q_steps, 0)

    def forward_q(g):
        q_to_mirror(g).wait_recv()
        q_forward(g).start()

    def k_steps(i, _):
        load_step(i, k_post)
        return 0
    lax.fori_loop(n_q + 1, n_q + n_kv + 1, k_steps, 0)

    def v_steps(i, _):
        load_step(i, v_post)
        forward_q(i - n_q - n_kv - 1)
        return 0
    lax.fori_loop(n_q + n_kv + 1, steps, v_steps, 0)
    v_post(steps - 1, cols[...])

    for h in range(heads):
        wide[0, pl.ds(h, rows, stride=heads), :] = k_new[h].astype(F32)
        wide[1, pl.ds(h, rows, stride=heads), :] = v_new[h].astype(F32).T
    k_out[...] = wide[0, 0:rows * heads, :].astype(BF16)
    v_out[...] = wide[1, 0:rows * heads, :].astype(BF16)

    def sibling_q(g, _):
        q_to_sibling(g).wait_recv()
        return 0
    lax.fori_loop(0, heads, sibling_q, 0)
    q_forward(0).wait_recv()
    q_forward(1).wait_recv()

    def sib_copy(kind, g):
        return remote(part.at[kind, g, 1], sib_recv.at[kind, g], sib_send.at[kind, g], sib_sem.at[kind, g], sibling)
    def mir_copy(g):
        return remote(comb.at[g], mir_recv.at[g], mir_send.at[g], mir_sem.at[g], mirror)

    def main_body():
        def q_cols(kind, g):
            base = 2 - 2 * kind
            return jnp.concatenate([qs[base, g], qs[base + 1, g]], axis=1)

        def dot(a, b):
            return lax.dot_general(a, b, (((1,), (0,)), ((), ())), preferred_element_type=F32)

        def col_max(mx, s):
            return jnp.maximum(mx, jnp.max(s.reshape(s.shape[0] // 8, 8, 512), axis=0))

        def qk(q, g, kc, slot, mx):
            s = dot(kh[g, pl.ds(pl.multiple_of(kc * KEY_TILE, KEY_TILE), KEY_TILE), :], q)
            SB[slot][kc] = s
            return col_max(mx, s)

        def qk_new(q, kind, g, slot, mx):
            own = lax.rem(me + 2 * (1 - kind), 4)
            other = lax.rem(sibling + 2 * (1 - kind), 4)
            key = lax.broadcasted_iota(jnp.int32, (rows, 512), 0) + me * rows
            col = lax.broadcasted_iota(jnp.int32, (rows, 512), 1)
            row = lax.rem(col, rows) + jnp.where(col < 256, own, other) * rows
            s = jnp.where(key <= row, dot(k_new[g], q), -jnp.inf)
            sN[slot] = s
            return col_max(mx, s)

        def weights(s, mc, ls):
            p = jnp.exp2(s * SCALE_LOG2 - mc)
            return p.astype(BF16), ls + jnp.sum(p.reshape(s.shape[0] // 8, 8, 512), axis=0)

        def block(last, kind_n, g_n, kind, g, b, par):
            steps = [("Q", i) for i in range(GROUP)] + [("Q", None)] * last
            for i in range(GROUP):
                steps.insert(LEAD + 2 * i, ("P", i))
            steps += [("P", None)] * last
            mx, ls, mc = mbuf[...], lbuf[...], mcb[par, 0:1, :]
            q = q_cols(kind_n, g_n)
            acc = None
            for op, i in steps:
                if op == "Q" and i is None:
                    mx = qk_new(q, kind_n, g_n, 1 - par, mx)
                elif op == "Q":
                    mx = qk(q, g_n, b * GROUP + i, 1 - par, mx)
                else:
                    if i is None:
                        p, ls = weights(sN[par], mc, ls)
                        v = v_new[g]
                    else:
                        kc = b * GROUP + i
                        p, ls = weights(SB[par][kc], mc, ls)
                        v = vt[g, :, pl.ds(pl.multiple_of(kc * KEY_TILE, KEY_TILE), KEY_TILE)]
                    pv = dot(v, p)
                    acc = pv if acc is None else acc + pv
            if not last:
                mbuf[...] = mx
                lbuf[...] = ls
                obuf[...] = acc
                return
            acc = obuf[...] + acc
            total = jnp.sum(ls, axis=0, keepdims=True)
            for t in range(2):
                part[kind, g, t, 0:128, :] = acc[:, TS(t)]
                part[kind, g, t, 128:129, :] = mc[:, TS(t)]
                part[kind, g, t, 129:130, :] = total[:, TS(t)]
            mcb[1 - par, 0:1, :] = jnp.max(mx, axis=0, keepdims=True) * SCALE_LOG2
            mbuf[...] = jnp.full(mbuf.shape, -jnp.inf, F32)
            lbuf[...] = jnp.zeros(lbuf.shape, F32)

        def merge(a, b):
            ma, mb = a[128:129, :], b[128:129, :]
            m = jnp.maximum(ma, mb)
            fa, fb = jnp.exp2(ma - m), jnp.exp2(mb - m)
            return a[0:128, :] * fa + b[0:128, :] * fb, m, a[129:130, :] * fa + b[129:130, :] * fb

        def send_merged(g):
            sib_copy(0, g).wait_recv()
            acc, m, total = merge(part.at[0, g, 0], sib_recv.at[0, g])
            comb[g, 0:128, :] = acc
            comb[g, 128:129, :] = m
            comb[g, 129:130, :] = total
            mir_copy(g).start()

        def unit_of(pos):
            half = pos // 2
            odd = pos - 2 * half
            local = jnp.where((odd == 1) & (half > 0) | (pos >= 2 * heads - 2), 1, 0)
            g = jnp.where(odd == 1, half - 1, half + 1)
            g = jnp.where(pos < 2, pos, jnp.where(pos >= 2 * heads - 2, pos - heads, g))
            return local, g

        def unit(p, par):
            pos = 2 * p + par
            kind, g = unit_of(pos)
            kind_n, g_n = unit_of(jnp.minimum(pos + 1, 2 * heads - 1))
            for b in range(tiles // GROUP):
                @pl.when(p < (2 + b) * heads)
                def _():
                    block(b == tiles // GROUP - 1, kind_n, g_n, kind, g, b, par)
                if b == 0:
                    @pl.when((p < heads - 1) if par else (p == 1))
                    def _():
                        send_merged(jnp.where(p == 0, 0, p + 1) if par else 1)
            sib_copy(kind, g).start()

        mbuf[...] = jnp.full(mbuf.shape, -jnp.inf, F32)
        q0 = q_cols(0, 0)
        def first(b, _):
            mx = mbuf[...]
            for c in range(16):
                mx = qk(q0, 0, 16 * b + c, 0, mx)
            mbuf[...] = mx
            return 0
        lax.fori_loop(0, tiles // 16, first, 0)
        mx = qk_new(q0, 0, 0, 0, mbuf[...])
        mcb[0, 0:1, :] = jnp.max(mx, axis=0, keepdims=True) * SCALE_LOG2
        mbuf[...] = jnp.full(mbuf.shape, -jnp.inf, F32)
        lbuf[...] = jnp.zeros(lbuf.shape, F32)

        def body(p, _):
            @pl.when(p + 3 < heads)
            def _():
                forward_q(p + 3)
            unit(p, 0)
            @pl.when(p + 2 < heads)
            def _():
                q_forward(p + 2).wait_recv()
            unit(p, 1)
            return 0
        lax.fori_loop(0, heads, body, 0)

        def final(g, _):
            sib_copy(1, g).wait_recv()
            mir_copy(g).wait_recv()
            acc, m, total = merge(part.at[1, g, 0], sib_recv.at[1, g])
            mb = mir_recv[g, 128:129, :]
            top = jnp.maximum(m, mb)
            fa, fb = jnp.exp2(m - top), jnp.exp2(mb - top)
            acc = acc * fa + mir_recv[g, 0:128, :] * fb
            total = total * fa + mir_recv[g, 129:130, :] * fb
            o = acc / total
            for j in range(2):
                cols = pl.ds(pl.multiple_of((2 * g + j) * 128, 128), 128)
                att[:, cols] = o[:, j * 128:(j + 1) * 128].T.astype(BF16)
            return 0
        lax.fori_loop(0, heads, final, 0)
        n_out = x_ref.shape[1] // 256
        def project(n, _):
            slot = lax.rem(n + steps, WSLOTS)
            weight_copy(w_o, n, slot).wait()
            cols = pl.ds(pl.multiple_of(n * 256, 256), 256)
            add = jnp.dot(att[...], wbuf[slot], preferred_element_type=F32)
            out_ref[:, cols] = (x_ref[:, cols].astype(F32) + add).astype(BF16)
            @pl.when(n + WSLOTS < n_out)
            def _():
                weight_copy(w_o, n + WSLOTS, slot).start()
            return 0
        lax.fori_loop(0, n_out, project, 0)

    main_body()

    def drain(g, _):
        q_to_mirror(g).wait_send()
        q_to_sibling(g).wait_send()
        q_forward(g).wait_send()
        sib_copy(0, g).wait_send()
        sib_copy(1, g).wait_send()
        mir_copy(g).wait_send()
        return 0
    lax.fori_loop(0, heads, drain, 0)


def attention_block(x, ln_gain, q_gain, k_gain, cos_tab, sin_tab, w_q, w_k, w_v, w_o, k_cache, v_cache):
    n_keys, heads, _ = k_cache.shape
    rows, width = x.shape
    vm = pl.BlockSpec(memory_space=pltpu.VMEM)
    hbm = pl.BlockSpec(memory_space=pl.ANY)
    dma = pltpu.SemaphoreType.DMA
    tiles = n_keys // KEY_TILE
    return pl.pallas_call(
        functools.partial(block_kernel, n_keys, heads),
        out_shape=(jax.ShapeDtypeStruct((rows, width), BF16), jax.ShapeDtypeStruct((rows * heads, HEAD_DIM), BF16),
                   jax.ShapeDtypeStruct((rows * heads, HEAD_DIM), BF16)),
        in_specs=[vm] * 6 + [hbm] * 6,
        out_specs=(vm, vm, vm),
        scratch_shapes=[
            pltpu.VMEM((rows, width), BF16), pltpu.VMEM((WSLOTS, width, 256), BF16),
            pltpu.VMEM((rows, 256), F32), pltpu.VMEM((rows, 128), F32), pltpu.VMEM((rows, 128), F32), pltpu.VMEM((rows, w_o.shape[0]), BF16),
            pltpu.VMEM((heads, rows, 128), BF16), pltpu.VMEM((heads, 128, rows), BF16),
            pltpu.VMEM((heads, n_keys, 128), BF16), pltpu.VMEM((heads, 128, n_keys), BF16),
            pltpu.VMEM((tiles, KEY_TILE, 512), F32), pltpu.VMEM((tiles, KEY_TILE, 512), F32),
            pltpu.VMEM((2, rows, 512), F32),
            pltpu.VMEM((8, 512), F32), pltpu.VMEM((8, 512), F32), pltpu.VMEM((2, 8, 512), F32), pltpu.VMEM((128, 512), F32),
            pltpu.VMEM((4, heads, 128, 256), BF16),
            pltpu.VMEM((2, heads, 2, 136, 256), F32), pltpu.VMEM((2, heads, 136, 256), F32),
            pltpu.VMEM((heads, 136, 256), F32), pltpu.VMEM((heads, 136, 256), F32),
            pltpu.VMEM((2, CSLOTS, PREP * heads, 128), BF16), pltpu.VMEM((2, PREP * heads, 128), F32),
            dma((2, CSLOTS)), dma((WSLOTS,)), dma((3, heads)), dma((3, heads)), dma((2, heads)), dma((2, heads)), dma((heads,)), dma((heads,)),
        ],
        compiler_params=pltpu.CompilerParams(vmem_limit_bytes=62 * 2**20, collective_id=0, has_side_effects=True),
    )(x, ln_gain, q_gain, k_gain, cos_tab, sin_tab, w_q, w_k, w_v, w_o,
      k_cache.reshape(n_keys * heads, HEAD_DIM), v_cache.reshape(n_keys * heads, HEAD_DIM))


def pass_on(*arrays):
    def kernel(*refs):
        n = len(refs) // 2
        for src, dst in zip(refs[:n], refs[n:]):
            dst[...] = src[...]
    vm = pl.BlockSpec(memory_space=pltpu.VMEM)
    return pl.pallas_call(kernel, out_shape=tuple(jax.ShapeDtypeStruct(a.shape, a.dtype) for a in arrays),
                          in_specs=[vm] * len(arrays), out_specs=(vm,) * len(arrays))(*arrays)


def solution(mesh):
    cp_size = mesh.shape['cp']
    row_spec = P(('dp', 'cp'), None)
    cache_spec = P(('dp', 'cp'), None, None)
    whole = P()

    def device_step(x_rows, k_cache, v_cache, ln_gain, w_q, w_k, w_v, w_o, q_gain, k_gain):
        rows = x_rows.shape[0]
        n_keys, heads, _ = k_cache.shape
        positions = n_keys * cp_size + lax.axis_index('cp') * rows + jnp.arange(rows)
        cos_tab, sin_tab = rope_tables(positions)
        out, k_new, v_new = pass_on(*attention_block(x_rows, ln_gain, q_gain, k_gain, cos_tab, sin_tab, w_q, w_k, w_v, w_o, k_cache, v_cache))
        return out, k_new.reshape(rows, heads, HEAD_DIM), v_new.reshape(rows, heads, HEAD_DIM)

    return jax.shard_map(device_step, mesh=mesh, in_specs=(row_spec, cache_spec, cache_spec, whole, whole, whole, whole, whole, whole, whole), out_specs=(row_spec, cache_spec, cache_spec), check_vma=False)
```
